128 devices in a mesh: dp: 1, cols: 16 (over z, y), rows: 8 (over x, core).
Axes of the slice: x: 4, y: 4, z: 4, core: 2. Of those that a mesh axis runs over, the one named last changes fastest.
Arguments:
- frames: bfloat16 [16, 1, 256, 512, 64], P(None, 'dp', 'rows', 'cols')
- w_in: bfloat16 [3, 3, 64, 768], replicated
- w_rec: bfloat16 [3, 3, 192, 768], replicated
- gate_bias: float32 [768], replicated
- h_init: bfloat16 [1, 256, 512, 192], P('dp', 'rows', 'cols')
- c_init: float32 [1, 256, 512, 192], P('dp', 'rows', 'cols')
Outputs:
- output 1: bfloat16 [16, 1, 256, 512, 192], P(None, 'dp', 'rows', 'cols')
- output 2: float32 [1, 256, 512, 192], P('dp', 'rows', 'cols')
All inputs are finite; a program needn't handle non-finite values.
Results may differ from the reference program's by a relative error of at most 0.00385845.
Values are sent between devices in bfloat16 or wider.
A program may use at most 1 GiB of HBM per device.

```python
import jax
import jax.numpy as jnp
from jax import lax

STEPS = 16
BATCH = 1
GRID_H = 256
GRID_W = 512
C_IN = 64
C_HID = 192

CONV_DIMS = ("NHWC", "HWIO", "NHWC")


def setup_inputs(seed: int = 0, part: int = 0) -> dict:
    part_key = jax.random.fold_in(jax.random.key(seed), part)
    k_frames, k_hid, k_cell = jax.random.split(part_key, 3)
    k_win, k_wrec, k_bias = jax.random.split(jax.random.key(seed + 1), 3)
    frames = jax.random.normal(k_frames, (STEPS, BATCH, GRID_H, GRID_W, C_IN), jnp.float32)
    w_in = jax.random.normal(k_win, (3, 3, C_IN, 4 * C_HID), jnp.float32) * (9 * C_IN) ** -0.5
    w_rec = jax.random.normal(k_wrec, (3, 3, C_HID, 4 * C_HID), jnp.float32) * (2.0 * (9 * C_HID) ** -0.5)
    forget_shift = jnp.concatenate([jnp.zeros((C_HID,), jnp.float32), jnp.ones((C_HID,), jnp.float32), jnp.zeros((2 * C_HID,), jnp.float32)])
    gate_bias = 0.5 * jax.random.normal(k_bias, (4 * C_HID,), jnp.float32) + forget_shift
    h_init = 0.5 * jax.random.normal(k_hid, (BATCH, GRID_H, GRID_W, C_HID), jnp.float32)
    c_init = jax.random.normal(k_cell, (BATCH, GRID_H, GRID_W, C_HID), jnp.float32)
    return {
        "frames": frames.astype(jnp.bfloat16),
        "w_in": w_in.astype(jnp.bfloat16),
        "w_rec": w_rec.astype(jnp.bfloat16),
        "gate_bias": gate_bias,
        "h_init": h_init.astype(jnp.bfloat16),
        "c_init": c_init,
    }


def conv_same(operand, kernel):
    return lax.conv_general_dilated(operand.astype(jnp.float32), kernel, (1, 1), "SAME", dimension_numbers=CONV_DIMS)


def reference(frames, w_in, w_rec, gate_bias, h_init, c_init):
    w_in32 = w_in.astype(jnp.float32)
    w_rec32 = w_rec.astype(jnp.float32)

    def time_step(carry_in, frame_t):
        h_prev, c_prev = carry_in
        gate_pre = conv_same(frame_t, w_in32) + conv_same(h_prev, w_rec32) + gate_bias
        gate_i, gate_f, gate_o, gate_g = jnp.split(gate_pre, 4, axis=-1)
        c_next = jax.nn.sigmoid(gate_f) * c_prev + jax.nn.sigmoid(gate_i) * jnp.tanh(gate_g)
        h_next = (jax.nn.sigmoid(gate_o) * jnp.tanh(c_next)).astype(jnp.bfloat16)
        return (h_next, c_next), h_next

    (h_last, c_last), hidden_seq = lax.scan(time_step, (h_init, c_init), frames)
    return hidden_seq, c_last
```

```python
import functools

import jax
import jax.numpy as jnp
from jax import lax
from jax.experimental import pallas as pl
from jax.experimental.pallas import tpu as pltpu
from jax.sharding import PartitionSpec as P

MESH = pl.DeviceIdType.MESH
F32, BF16 = jnp.float32, jnp.bfloat16

STEPS = 16
TILE = 32
C_IN, C_HID = 64, 192
LANES = 128
PITCH = 48
ROW_SETS = (range(1, 9), range(9, 17), range(17, 25), (*range(25, 31), 0, 31))

UP, DOWN, LEFT, RIGHT = (-1, 0), (1, 0), (0, -1), (0, 1)
DIRS = (UP, DOWN, LEFT, RIGHT, (-1, -1), (-1, 1), (1, -1), (1, 1))


def sigmoid(x):
    return 0.5 * jnp.tanh(0.5 * x) + 0.5


def kernel(n_rows, n_cols, frames, w_in, w_rec, bias, h_init, c_init, hidden, c_out,
         w, lhs, st0, st1, c0, c1, ge, ce, cv, fb, ob, ci, cs, row_in, col_in, diag_in,
         send_sem, recv_sem, frame_sem, out_sem, load_sem):
    my_row, my_col = lax.axis_index("rows"), lax.axis_index("cols")

    def there(d):
        r, c = my_row + d[0], my_col + d[1]
        return (r >= 0) & (r < n_rows) & (c >= 0) & (c < n_cols)

    def device(d):
        return {"rows": my_row + d[0], "cols": my_col + d[1]}

    load_w0 = pltpu.make_async_copy(w_rec, w.at[:, 0:C_HID, :], load_sem.at[0])
    load_w1 = pltpu.make_async_copy(w_in, w.at[:, C_HID:256, :], load_sem.at[1])
    load_h = pltpu.make_async_copy(h_init, ob.at[0], load_sem.at[2])
    load_c = pltpu.make_async_copy(c_init, ci, load_sem.at[3])

    def frame_copy(t, slot):
        return pltpu.make_async_copy(frames.at[t], fb.at[slot], frame_sem.at[slot])

    def out_copy(t, slot):
        return pltpu.make_async_copy(ob.at[slot], hidden.at[t], out_sem.at[slot])

    load_h.start()
    frame_copy(0, 0).start()
    load_c.start()
    load_w0.start()
    load_w1.start()
    frame_copy(1, 1).start()

    row_in[...] = jnp.zeros_like(row_in)
    col_in[...] = jnp.zeros_like(col_in)
    diag_in[...] = jnp.zeros_like(diag_in)
    for k in range(TILE + 2):
        for st in (st0, st1):
            st[pl.ds(k * PITCH, 8), :] = jnp.zeros((8, LANES), F32)
            st[pl.ds(k * PITCH + 40, 8), :] = jnp.zeros((8, LANES), F32)

    barrier = pltpu.get_barrier_semaphore()
    for d in DIRS:
        @pl.when(there(d))
        def _():
            pl.semaphore_signal(barrier, inc=1, device_id=device(d), device_id_type=MESH)
    def near(i, n):
        return 1 + (i > 0).astype(jnp.int32) + (i < n - 1).astype(jnp.int32)

    pl.semaphore_wait(barrier, near(my_row, n_rows) * near(my_col, n_cols) - 1)

    lane = lax.broadcasted_iota(jnp.int32, (TILE, LANES), 1)
    low = lane < C_IN

    def frame_row(slot, r):
        x = fb[slot, r].astype(F32)
        return jnp.concatenate([x, x], axis=1)

    load_h.wait()
    frame_copy(0, 0).wait()
    for r in range(TILE):
        st0[pl.ds(r * PITCH + 8, TILE), :] = ob[0, r, :, 0:LANES].astype(F32)
        h1 = ob[0, r, :, LANES:C_HID].astype(F32)
        st1[pl.ds(r * PITCH + 8, TILE), :] = jnp.where(low, jnp.concatenate([h1, h1], axis=1), frame_row(0, r))
    load_c.wait()
    for r in range(TILE):
        c0[pl.ds(r * TILE, TILE), :] = ci[r, :, 0:LANES]
        v = ci[r, :, LANES:C_HID]
        c1[pl.ds(r * TILE, TILE), :] = jnp.concatenate([v, v], axis=1)
    for side in range(2):
        ce[side, 0] = c0[pl.ds((TILE - 1) * side, TILE, stride=TILE), :]
        ce[side, 1] = c1[pl.ds((TILE - 1) * side, TILE, stride=TILE), :]
    load_w0.wait()
    load_w1.wait()

    def build_row(r, out_slot):
        target = r + 1 if r < TILE else (0 if r == TILE else TILE + 1)
        for dx in range(3):
            v0 = st0[pl.ds(r * PITCH + 7 + dx, TILE), :].astype(BF16)
            v1 = st1[pl.ds(r * PITCH + 7 + dx, TILE), :].astype(BF16)
            lhs[dx, target, :, 0:LANES] = v0
            lhs[dx, target, :, LANES:256] = v1
            if dx == 1 and out_slot is not None:
                ob[out_slot, r, :, 0:LANES] = v0
                ob[out_slot, r, :, LANES:C_HID] = v1[:, 0:C_IN]

    def cell(gates, c0_prev, c1_prev):
        s0, s1, s2, s3 = (sigmoid(gates[k]) for k in range(4))
        scale = jnp.where(low, 0.5, 1.0)
        t4 = jnp.tanh(gates[4] * scale) * scale + jnp.where(low, 0.5, 0.0)
        t5 = jnp.tanh(gates[5])
        r1, r2, r4, r5 = (pltpu.roll(v, 64, 1) for v in (s1, s2, t4, t5))
        c0_next = jnp.where(low, r1, r2) * c0_prev + s0 * jnp.where(low, r4, r5)
        c1_next = r2 * c1_prev + s1 * r5
        return s3 * jnp.tanh(c0_next), t4 * jnp.tanh(c1_next), c0_next, c1_next

    def bias_piece(k):
        return bias[:, k * LANES:(k + 1) * LANES]

    def chunk_gates(rows):
        x = [jnp.concatenate([lhs[dx, r + dy] for r in rows], axis=0) for dy in range(3) for dx in range(3)]
        return jnp.dot(jnp.concatenate(x, axis=1), w[...].reshape(9 * 256, 4 * C_HID), preferred_element_type=F32)

    def cell_row(gates, j, r, x_slot):
        pre = gates[j * TILE:(j + 1) * TILE]
        pre = [pre[:, k * LANES:(k + 1) * LANES] + bias_piece(k) for k in range(6)]
        for k in range(6):
            ge[0, k, pl.ds(r * 8, 8), :] = pre[k][0:8]
            ge[1, k, pl.ds(r * 8, 8), :] = pre[k][24:32]
        at = pl.ds(r * TILE, TILE)
        h0, h1, c0_next, c1_next = cell(pre, c0[at, :], c1[at, :])
        c0[at, :] = c0_next
        c1[at, :] = c1_next
        st0[pl.ds(r * PITCH + 8, TILE), :] = h0
        st1[pl.ds(r * PITCH + 8, TILE), :] = jnp.where(low, h1, frame_row(x_slot, r))

    def sends(slot):
        pieces = (
            (UP, lhs.at[1, 1], row_in.at[slot, 1]),
            (DOWN, lhs.at[1, TILE], row_in.at[slot, 0]),
            (LEFT, cs.at[0], col_in.at[slot, 1]),
            (RIGHT, cs.at[1], col_in.at[slot, 0]),
            ((-1, -1), cs.at[0, 0:16], diag_in.at[slot, 3]),
            ((-1, 1), cs.at[1, 0:16], diag_in.at[slot, 2]),
            ((1, -1), cs.at[0, 16:32], diag_in.at[slot, 1]),
            ((1, 1), cs.at[1, 16:32], diag_in.at[slot, 0]),
        )
        return [(d, pltpu.make_async_remote_copy(
            src_ref=src, dst_ref=dst, send_sem=send_sem.at[slot, k], recv_sem=recv_sem.at[slot, k],
            device_id=device(d), device_id_type=MESH)) for k, (d, src, dst) in enumerate(pieces)]

    def wait_recv(copies, which):
        for k in which:
            d, copy = copies[k]
            @pl.when(there((-d[0], -d[1])))
            def _():
                copy.wait_recv()

    def step(t, _):
        slot = lax.rem(t, 2)
        x_slot = lax.rem(t + 1, 2)
        copies = sends(slot)

        @pl.when(t >= 3)
        def _():
            out_copy(t - 3, x_slot).wait()

        for side in range(2):
            at = pl.ds(8 + (TILE - 1) * side, TILE, stride=PITCH)
            cs[side, :, 0:LANES] = st0[at, :].astype(BF16)
            cs[side, :, LANES:256] = st1[at, :].astype(BF16)
        build_row(0, x_slot)
        build_row(TILE - 1, x_slot)
        for d, copy in copies:
            @pl.when(there(d))
            def _():
                copy.start()

        @pl.when(t < STEPS - 1)
        def _():
            frame_copy(t + 1, x_slot).wait()

        for r in range(1, 10):
            build_row(r, x_slot)
        gates = chunk_gates(ROW_SETS[0])
        for r in range(10, 18):
            build_row(r, x_slot)
        more = chunk_gates(ROW_SETS[1])
        for j, r in enumerate(ROW_SETS[0]):
            cell_row(gates, j, r, x_slot)
        for r in range(18, 31):
            build_row(r, x_slot)
        gates = chunk_gates(ROW_SETS[2])
        for j, r in enumerate(ROW_SETS[1]):
            cell_row(more, j, r, x_slot)
        for j, r in enumerate(ROW_SETS[2]):
            cell_row(gates, j, r, x_slot)

        wait_recv(copies, (0, 1))
        @pl.when(t >= 1)
        def _():
            out_copy(t - 1, x_slot).start()
        @pl.when(t < STEPS - 2)
        def _():
            frame_copy(t + 2, slot).start()
        for k in range(2):
            at = pl.ds((TILE + k) * PITCH + 8, TILE)
            st0[at, :] = row_in[slot, k, :, 0:LANES].astype(F32)
            st1[at, :] = row_in[slot, k, :, LANES:256].astype(F32)
            build_row(TILE + k, None)
        gates = chunk_gates(ROW_SETS[3])

        wait_recv(copies, range(2, 8))
        for side in range(2):
            for k in range(2):
                part = slice(k * LANES, (k + 1) * LANES)
                cv[side, k, 8:40, :] = col_in[slot, side, :, part].astype(F32)
                cv[side, k, 7:8, :] = diag_in[slot, side, 15:16, part].astype(F32)
                cv[side, k, 40:41, :] = diag_in[slot, 2 + side, 0:1, part].astype(F32)
        extra = []
        for side in range(2):
            halo = jnp.concatenate([cv[side, k, 7 + dy:39 + dy, :].astype(BF16) for dy in range(3) for k in range(2)], axis=1)
            taps = jnp.concatenate([w[dy * 3 + 2 * side] for dy in range(3)], axis=0)
            extra.append(jnp.dot(halo, taps, preferred_element_type=F32))
        for j, r in enumerate(ROW_SETS[3]):
            cell_row(gates, j, r, x_slot)
        for side in range(2):
            more = [extra[side][:, k * LANES:(k + 1) * LANES] for k in range(6)]
            pre = [ge[side, k, pl.ds(7 * side, TILE, stride=8), :] + more[k] for k in range(6)]
            h0, h1, c0_next, c1_next = cell(pre, ce[side, 0], ce[side, 1])
            ce[side, 0] = c0_next
            ce[side, 1] = c1_next
            at = pl.ds(8 + (TILE - 1) * side, TILE, stride=PITCH)
            st0[at, :] = h0
            st1[at, :] = jnp.where(low, h1, st1[at, :])
        for d, copy in copies:
            @pl.when(there(d))
            def _():
                copy.wait_send()
        return 0

    lax.fori_loop(0, STEPS, step, 0)

    out_copy(STEPS - 3, 1).wait()
    for r in range(TILE):
        at = pl.ds(r * PITCH + 8, TILE)
        ob[1, r, :, 0:LANES] = st0[at, :].astype(BF16)
        ob[1, r, :, LANES:C_HID] = st1[at, :].astype(BF16)[:, 0:C_IN]
    out_copy(STEPS - 1, 1).start()
    for side in range(2):
        c0[pl.ds((TILE - 1) * side, TILE, stride=TILE), :] = ce[side, 0]
        c1[pl.ds((TILE - 1) * side, TILE, stride=TILE), :] = ce[side, 1]
    for r in range(TILE):
        at = pl.ds(r * TILE, TILE)
        ci[r, :, 0:LANES] = c0[at, :]
        ci[r, :, LANES:C_HID] = c1[at, :][:, 0:C_IN]
    store_c = pltpu.make_async_copy(ci, c_out, load_sem.at[3])
    store_c.start()
    out_copy(STEPS - 2, 0).wait()
    out_copy(STEPS - 1, 1).wait()
    store_c.wait()


def solution(mesh):
    n_rows = mesh.shape["rows"]
    n_cols = mesh.shape["cols"]
    seq_spec = P(None, "dp", "rows", "cols", None)
    state_spec = P("dp", "rows", "cols", None)

    def local_run(frames, w_in, w_rec, gate_bias, h_init, c_init):
        frames = frames.reshape(STEPS, TILE, TILE, C_IN)
        w_in = w_in.reshape(9, C_IN, 4 * C_HID)
        w_rec = w_rec.reshape(9, C_HID, 4 * C_HID)
        bias = gate_bias.reshape(1, 4 * C_HID)
        h_init = h_init.reshape(TILE, TILE, C_HID)
        c_init = c_init.reshape(TILE, TILE, C_HID)
        hbm = pl.BlockSpec(memory_space=pltpu.HBM)
        vmem = pl.BlockSpec(memory_space=pltpu.VMEM)
        dma = pltpu.SemaphoreType.DMA
        hidden, c_last = pl.pallas_call(
            functools.partial(kernel, n_rows, n_cols),
            out_shape=(
                jax.ShapeDtypeStruct((STEPS, TILE, TILE, C_HID), BF16),
                jax.ShapeDtypeStruct((TILE, TILE, C_HID), F32),
            ),
            in_specs=[hbm, hbm, hbm, vmem, hbm, hbm],
            out_specs=(hbm, hbm),
            scratch_shapes=[
                pltpu.VMEM((9, 256, 4 * C_HID), BF16),
                pltpu.VMEM((3, TILE + 2, TILE, 256), BF16),
                pltpu.VMEM(((TILE + 2) * PITCH, LANES), F32),
                pltpu.VMEM(((TILE + 2) * PITCH, LANES), F32),
                pltpu.VMEM((TILE * TILE, LANES), F32),
                pltpu.VMEM((TILE * TILE, LANES), F32),
                pltpu.VMEM((2, 6, 8 * TILE, LANES), F32),
                pltpu.VMEM((2, 2, TILE, LANES), F32),
                pltpu.VMEM((2, 2, PITCH, LANES), F32),
                pltpu.VMEM((2, TILE, TILE, C_IN), BF16),
                pltpu.VMEM((2, TILE, TILE, C_HID), BF16),
                pltpu.VMEM((TILE, TILE, C_HID), F32),
                pltpu.VMEM((2, TILE, 256), BF16),
                pltpu.VMEM((2, 2, TILE, 256), BF16),
                pltpu.VMEM((2, 2, TILE, 256), BF16),
                pltpu.VMEM((2, 4, 16, 256), BF16),
                dma((2, 8)), dma((2, 8)), dma((2,)), dma((2,)), dma((4,)),
            ],
            compiler_params=pltpu.CompilerParams(collective_id=0, has_side_effects=True, vmem_limit_bytes=56 * 1024 * 1024),
        )(frames, w_in, w_rec, bias, h_init, c_init)
        return hidden.reshape(STEPS, 1, TILE, TILE, C_HID), c_last.reshape(1, TILE, TILE, C_HID)

    return jax.shard_map(local_run, mesh=mesh, in_specs=(seq_spec, P(), P(), P(), state_spec, state_spec), out_specs=(seq_spec, state_spec), check_vma=False)
```

```python
import functools

import jax
import jax.numpy as jnp
from jax import lax
from jax.experimental import pallas as pl
from jax.experimental.pallas import tpu as pltpu
from jax.sharding import PartitionSpec as P

MESH = pl.DeviceIdType.MESH
F32, BF16 = jnp.float32, jnp.bfloat16

STEPS = 16
TILE = 32
C_IN, C_HID = 64, 192
LANES = 128
PITCH = 48
ROW_SETS = (range(1, 9), range(9, 17), range(17, 25), (*range(25, 31), 0, 31))

UP, DOWN, LEFT, RIGHT = (-1, 0), (1, 0), (0, -1), (0, 1)
DIRS = (UP, DOWN, LEFT, RIGHT, (-1, -1), (-1, 1), (1, -1), (1, 1))


def sigmoid(x):
    return 0.5 * jnp.tanh(0.5 * x) + 0.5


def kernel(n_rows, n_cols, frames, w_in, w_rec, bias, h_init, c_init, hidden, c_out,
         w, lhs, st0, st1, c0, c1, ge, ce, cv, fb, hb, bb, ci, cs, row_in, col_in, diag_in,
         send_sem, recv_sem, frame_sem, load_sem):
    my_row, my_col = lax.axis_index("rows"), lax.axis_index("cols")

    def there(d):
        r, c = my_row + d[0], my_col + d[1]
        return (r >= 0) & (r < n_rows) & (c >= 0) & (c < n_cols)

    def device(d):
        return {"rows": my_row + d[0], "cols": my_col + d[1]}

    load_w0 = pltpu.make_async_copy(w_rec, w.at[:, 0:C_HID, :], load_sem.at[0])
    load_w1 = pltpu.make_async_copy(w_in, w.at[:, C_HID:256, :], load_sem.at[1])
    load_h = pltpu.make_async_copy(h_init, hb, load_sem.at[2])
    load_c = pltpu.make_async_copy(c_init, ci, load_sem.at[3])

    def frame_copy(t, slot):
        return pltpu.make_async_copy(frames.at[t], fb.at[slot], frame_sem.at[slot])

    load_b = pltpu.make_async_copy(bias, bb, load_sem.at[4])
    load_h.start()
    load_b.start()
    frame_copy(0, 0).start()
    load_c.start()
    load_w0.start()
    load_w1.start()
    frame_copy(1, 1).start()

    row_in[...] = jnp.zeros_like(row_in)
    col_in[...] = jnp.zeros_like(col_in)
    diag_in[...] = jnp.zeros_like(diag_in)
    for k in range(TILE + 2):
        for st in (st0, st1):
            st[pl.ds(k * PITCH, 8), :] = jnp.zeros((8, LANES), F32)
            st[pl.ds(k * PITCH + 40, 8), :] = jnp.zeros((8, LANES), F32)

    barrier = pltpu.get_barrier_semaphore()
    for d in DIRS:
        @pl.when(there(d))
        def _():
            pl.semaphore_signal(barrier, inc=1, device_id=device(d), device_id_type=MESH)
    def near(i, n):
        return 1 + (i > 0).astype(jnp.int32) + (i < n - 1).astype(jnp.int32)

    pl.semaphore_wait(barrier, near(my_row, n_rows) * near(my_col, n_cols) - 1)

    lane = lax.broadcasted_iota(jnp.int32, (TILE, LANES), 1)
    low = lane < C_IN

    def frame_row(slot, r):
        x = fb[slot, r].astype(F32)
        return jnp.concatenate([x, x], axis=1)

    load_h.wait()
    frame_copy(0, 0).wait()
    for r in range(TILE):
        st0[pl.ds(r * PITCH + 8, TILE), :] = hb[r, :, 0:LANES].astype(F32)
        h1 = hb[r, :, LANES:C_HID].astype(F32)
        st1[pl.ds(r * PITCH + 8, TILE), :] = jnp.where(low, jnp.concatenate([h1, h1], axis=1), frame_row(0, r))
    load_b.wait()
    load_c.wait()
    for r in range(TILE):
        c0[pl.ds(r * TILE, TILE), :] = ci[r, :, 0:LANES]
        v = ci[r, :, LANES:C_HID]
        c1[pl.ds(r * TILE, TILE), :] = jnp.concatenate([v, v], axis=1)
    for side in range(2):
        ce[side, 0] = c0[pl.ds((TILE - 1) * side, TILE, stride=TILE), :]
        ce[side, 1] = c1[pl.ds((TILE - 1) * side, TILE, stride=TILE), :]
    load_w0.wait()
    load_w1.wait()

    def build_row(r, out_slot):
        target = r + 1 if r < TILE else (0 if r == TILE else TILE + 1)
        for dx in range(3):
            v0 = st0[pl.ds(r * PITCH + 7 + dx, TILE), :].astype(BF16)
            v1 = st1[pl.ds(r * PITCH + 7 + dx, TILE), :].astype(BF16)
            lhs[dx, target, :, 0:LANES] = v0
            lhs[dx, target, :, LANES:256] = v1
            if dx == 1 and out_slot is not None:
                hidden[out_slot, r, :, 0:LANES] = v0
                hidden[out_slot, r, :, LANES:C_HID] = v1[:, 0:C_IN]

    def cell(gates, c0_prev, c1_prev):
        s0, s1, s2, s3 = (sigmoid(gates[k]) for k in range(4))
        scale = jnp.where(low, 0.5, 1.0)
        t4 = jnp.tanh(gates[4] * scale) * scale + jnp.where(low, 0.5, 0.0)
        t5 = jnp.tanh(gates[5])
        r1, r2, r4, r5 = (pltpu.roll(v, 64, 1) for v in (s1, s2, t4, t5))
        c0_next = jnp.where(low, r1, r2) * c0_prev + s0 * jnp.where(low, r4, r5)
        c1_next = r2 * c1_prev + s1 * r5
        return s3 * jnp.tanh(c0_next), t4 * jnp.tanh(c1_next), c0_next, c1_next

    def bias_piece(k):
        return bb[k * LANES:(k + 1) * LANES].reshape(1, LANES)

    def chunk_gates(rows):
        x = [jnp.concatenate([lhs[dx, r + dy] for r in rows], axis=0) for dy in range(3) for dx in range(3)]
        return jnp.dot(jnp.concatenate(x, axis=1), w[...].reshape(9 * 256, 4 * C_HID), preferred_element_type=F32)

    def cell_row(gates, j, r, x_slot):
        pre = gates[j * TILE:(j + 1) * TILE]
        pre = [pre[:, k * LANES:(k + 1) * LANES] + bias_piece(k) for k in range(6)]
        for k in range(6):
            ge[0, k, pl.ds(r * 8, 8), :] = pre[k][0:8]
            ge[1, k, pl.ds(r * 8, 8), :] = pre[k][24:32]
        at = pl.ds(r * TILE, TILE)
        h0, h1, c0_next, c1_next = cell(pre, c0[at, :], c1[at, :])
        c0[at, :] = c0_next
        c1[at, :] = c1_next
        st0[pl.ds(r * PITCH + 8, TILE), :] = h0
        st1[pl.ds(r * PITCH + 8, TILE), :] = jnp.where(low, h1, frame_row(x_slot, r))

    def sends(slot):
        pieces = (
            (UP, lhs.at[1, 1], row_in.at[slot, 1]),
            (DOWN, lhs.at[1, TILE], row_in.at[slot, 0]),
            (LEFT, cs.at[0], col_in.at[slot, 1]),
            (RIGHT, cs.at[1], col_in.at[slot, 0]),
            ((-1, -1), cs.at[0, 0:16], diag_in.at[slot, 3]),
            ((-1, 1), cs.at[1, 0:16], diag_in.at[slot, 2]),
            ((1, -1), cs.at[0, 16:32], diag_in.at[slot, 1]),
            ((1, 1), cs.at[1, 16:32], diag_in.at[slot, 0]),
        )
        return [(d, pltpu.make_async_remote_copy(
            src_ref=src, dst_ref=dst, send_sem=send_sem.at[slot, k], recv_sem=recv_sem.at[slot, k],
            device_id=device(d), device_id_type=MESH)) for k, (d, src, dst) in enumerate(pieces)]

    def wait_recv(copies, which):
        for k in which:
            d, copy = copies[k]
            @pl.when(there((-d[0], -d[1])))
            def _():
                copy.wait_recv()

    def step(t, _):
        slot = lax.rem(t, 2)
        x_slot = lax.rem(t + 1, 2)
        copies = sends(slot)

        done = lax.rem(t + STEPS - 1, STEPS)
        for side in range(2):
            at = pl.ds(8 + (TILE - 1) * side, TILE, stride=PITCH)
            cs[side, :, 0:LANES] = st0[at, :].astype(BF16)
            cs[side, :, LANES:256] = st1[at, :].astype(BF16)
        build_row(0, done)
        build_row(TILE - 1, done)
        for d, copy in copies:
            @pl.when(there(d))
            def _():
                copy.start()

        @pl.when(t < STEPS - 1)
        def _():
            frame_copy(t + 1, x_slot).wait()

        for r in range(1, 10):
            build_row(r, done)
        gates = chunk_gates(ROW_SETS[0])
        for r in range(10, 18):
            build_row(r, done)
        more = chunk_gates(ROW_SETS[1])
        for j, r in enumerate(ROW_SETS[0]):
            cell_row(gates, j, r, x_slot)
        for r in range(18, 31):
            build_row(r, done)
        gates = chunk_gates(ROW_SETS[2])
        for j, r in enumerate(ROW_SETS[1]):
            cell_row(more, j, r, x_slot)
        wait_recv(copies, (0, 1))
        @pl.when(t < STEPS - 2)
        def _():
            frame_copy(t + 2, slot).start()
        for k in range(2):
            at = pl.ds((TILE + k) * PITCH + 8, TILE)
            st0[at, :] = row_in[slot, k, :, 0:LANES].astype(F32)
            st1[at, :] = row_in[slot, k, :, LANES:256].astype(F32)
            build_row(TILE + k, None)
        more = chunk_gates(ROW_SETS[3])
        for j, r in enumerate(ROW_SETS[2]):
            cell_row(gates, j, r, x_slot)

        wait_recv(copies, range(2, 8))
        for side in range(2):
            for k in range(2):
                part = slice(k * LANES, (k + 1) * LANES)
                cv[side, k, 8:40, :] = col_in[slot, side, :, part].astype(F32)
                cv[side, k, 7:8, :] = diag_in[slot, side, 15:16, part].astype(F32)
                cv[side, k, 40:41, :] = diag_in[slot, 2 + side, 0:1, part].astype(F32)
        extra = []
        for side in range(2):
            halo = jnp.concatenate([cv[side, k, 7 + dy:39 + dy, :].astype(BF16) for dy in range(3) for k in range(2)], axis=1)
            taps = jnp.concatenate([w[dy * 3 + 2 * side] for dy in range(3)], axis=0)
            extra.append(jnp.dot(halo, taps, preferred_element_type=F32))
        for j, r in enumerate(ROW_SETS[3]):
            cell_row(more, j, r, x_slot)
        for side in range(2):
            more = [extra[side][:, k * LANES:(k + 1) * LANES] for k in range(6)]
            pre = [ge[side, k, pl.ds(7 * side, TILE, stride=8), :] + more[k] for k in range(6)]
            h0, h1, c0_next, c1_next = cell(pre, ce[side, 0], ce[side, 1])
            ce[side, 0] = c0_next
            ce[side, 1] = c1_next
            at = pl.ds(8 + (TILE - 1) * side, TILE, stride=PITCH)
            st0[at, :] = h0
            st1[at, :] = jnp.where(low, h1, st1[at, :])
        for d, copy in copies:
            @pl.when(there(d))
            def _():
                copy.wait_send()
        return 0

    lax.fori_loop(0, STEPS, step, 0)

    for r in range(TILE):
        at = pl.ds(r * PITCH + 8, TILE)
        hidden[STEPS - 1, r, :, 0:LANES] = st0[at, :].astype(BF16)
        hidden[STEPS - 1, r, :, LANES:C_HID] = st1[at, :].astype(BF16)[:, 0:C_IN]
    for side in range(2):
        c0[pl.ds((TILE - 1) * side, TILE, stride=TILE), :] = ce[side, 0]
        c1[pl.ds((TILE - 1) * side, TILE, stride=TILE), :] = ce[side, 1]
    for r in range(TILE):
        at = pl.ds(r * TILE, TILE)
        c_out[r, :, 0:LANES] = c0[at, :]
        c_out[r, :, LANES:C_HID] = c1[at, :][:, 0:C_IN]


def solution(mesh):
    n_rows = mesh.shape["rows"]
    n_cols = mesh.shape["cols"]
    seq_spec = P(None, "dp", "rows", "cols", None)
    state_spec = P("dp", "rows", "cols", None)

    def local_run(frames, w_in, w_rec, gate_bias, h_init, c_init):
        frames = frames.reshape(STEPS, TILE, TILE, C_IN)
        w_in = w_in.reshape(9, C_IN, 4 * C_HID)
        w_rec = w_rec.reshape(9, C_HID, 4 * C_HID)
        h_init = h_init.reshape(TILE, TILE, C_HID)
        c_init = c_init.reshape(TILE, TILE, C_HID)
        hbm = pl.BlockSpec(memory_space=pltpu.HBM)
        vmem = pl.BlockSpec(memory_space=pltpu.VMEM)
        dma = pltpu.SemaphoreType.DMA
        hidden, c_last = pl.pallas_call(
            functools.partial(kernel, n_rows, n_cols),
            out_shape=(
                pltpu.VMEM((STEPS, TILE, TILE, C_HID), BF16),
                pltpu.VMEM((TILE, TILE, C_HID), F32),
            ),
            in_specs=[hbm] * 6,
            out_specs=(vmem, vmem),
            scratch_shapes=[
                pltpu.VMEM((9, 256, 4 * C_HID), BF16),
                pltpu.VMEM((3, TILE + 2, TILE, 256), BF16),
                pltpu.VMEM(((TILE + 2) * PITCH, LANES), F32),
                pltpu.VMEM(((TILE + 2) * PITCH, LANES), F32),
                pltpu.VMEM((TILE * TILE, LANES), F32),
                pltpu.VMEM((TILE * TILE, LANES), F32),
                pltpu.VMEM((2, 6, 8 * TILE, LANES), F32),
                pltpu.VMEM((2, 2, TILE, LANES), F32),
                pltpu.VMEM((2, 2, PITCH, LANES), F32),
                pltpu.VMEM((2, TILE, TILE, C_IN), BF16),
                pltpu.VMEM((TILE, TILE, C_HID), BF16),
                pltpu.VMEM((4 * C_HID,), F32),
                pltpu.VMEM((TILE, TILE, C_HID), F32),
                pltpu.VMEM((2, TILE, 256), BF16),
                pltpu.VMEM((2, 2, TILE, 256), BF16),
                pltpu.VMEM((2, 2, TILE, 256), BF16),
                pltpu.VMEM((2, 4, 16, 256), BF16),
                dma((2, 8)), dma((2, 8)), dma((2,)), dma((5,)),
            ],
            compiler_params=pltpu.CompilerParams(collective_id=0, has_side_effects=True, vmem_limit_bytes=52 * 1024 * 1024),
        )(frames, w_in, w_rec, gate_bias, h_init, c_init)
        return hidden.reshape(STEPS, 1, TILE, TILE, C_HID), c_last.reshape(1, TILE, TILE, C_HID)

    return jax.shard_map(local_run, mesh=mesh, in_specs=(seq_spec, P(), P(), P(), state_spec, state_spec), out_specs=(seq_spec, state_spec), check_vma=False)
```

```python
import functools

import jax
import jax.numpy as jnp
from jax import lax
from jax.experimental import pallas as pl
from jax.experimental.pallas import tpu as pltpu
from jax.sharding import PartitionSpec as P

MESH = pl.DeviceIdType.MESH
F32, BF16 = jnp.float32, jnp.bfloat16

STEPS = 16
TILE = 32
C_IN, C_HID = 64, 192
LANES = 128
PITCH = 48
ROW_SETS = (range(1, 9), range(9, 17), range(17, 25), (*range(25, 31), 0, 31))
HALVES = (2, 2, 2, 2)
LATE = 6

UP, DOWN, LEFT, RIGHT = (-1, 0), (1, 0), (0, -1), (0, 1)
DIRS = (UP, DOWN, LEFT, RIGHT, (-1, -1), (-1, 1), (1, -1), (1, 1))


def sigmoid(x):
    return 0.5 * jnp.tanh(0.5 * x) + 0.5


def kernel(n_rows, n_cols, frames, w_in, w_rec, bias, h_init, c_init, hidden, c_out,
         w, lhs, st0, st1, c0, c1, ge, gp, ce, cv, fb, hb, bb, ci, cs, row_in, col_in, diag_in,
         send_sem, recv_sem, frame_sem, load_sem):
    my_row, my_col = lax.axis_index("rows"), lax.axis_index("cols")

    def there(d):
        r, c = my_row + d[0], my_col + d[1]
        return (r >= 0) & (r < n_rows) & (c >= 0) & (c < n_cols)

    def device(d):
        return {"rows": my_row + d[0], "cols": my_col + d[1]}

    load_w0 = pltpu.make_async_copy(w_rec, w.at[:, 0:C_HID, :], load_sem.at[0])
    load_w1 = pltpu.make_async_copy(w_in, w.at[:, C_HID:256, :], load_sem.at[1])
    load_h = pltpu.make_async_copy(h_init, hb, load_sem.at[2])
    load_c = pltpu.make_async_copy(c_init, ci, load_sem.at[3])

    def frame_copy(t, slot):
        return pltpu.make_async_copy(frames.at[t], fb.at[slot], frame_sem.at[slot])

    load_b = pltpu.make_async_copy(bias, bb, load_sem.at[4])
    load_h.start()
    load_b.start()
    frame_copy(0, 0).start()
    load_c.start()
    load_w0.start()
    load_w1.start()
    frame_copy(1, 1).start()

    row_in[...] = jnp.zeros_like(row_in)
    col_in[...] = jnp.zeros_like(col_in)
    diag_in[...] = jnp.zeros_like(diag_in)
    gp[...] = jnp.zeros_like(gp)
    for k in range(TILE + 2):
        for st in (st0, st1):
            st[pl.ds(k * PITCH, 8), :] = jnp.zeros((8, LANES), F32)
            st[pl.ds(k * PITCH + 40, 8), :] = jnp.zeros((8, LANES), F32)

    barrier = pltpu.get_barrier_semaphore()
    for d in DIRS:
        @pl.when(there(d))
        def _():
            pl.semaphore_signal(barrier, inc=1, device_id=device(d), device_id_type=MESH)
    def near(i, n):
        return 1 + (i > 0).astype(jnp.int32) + (i < n - 1).astype(jnp.int32)

    pl.semaphore_wait(barrier, near(my_row, n_rows) * near(my_col, n_cols) - 1)

    lane = lax.broadcasted_iota(jnp.int32, (TILE, LANES), 1)
    low = lane < C_IN
    cell_at = lax.broadcasted_iota(jnp.int32, (TILE, LANES), 0)

    def frame_row(slot, r):
        x = fb[slot, r].astype(F32)
        return jnp.concatenate([x, x], axis=1)

    load_h.wait()
    frame_copy(0, 0).wait()
    for r in range(TILE):
        st0[pl.ds(r * PITCH + 8, TILE), :] = hb[r, :, 0:LANES].astype(F32)
        h1 = hb[r, :, LANES:C_HID].astype(F32)
        st1[pl.ds(r * PITCH + 8, TILE), :] = jnp.where(low, jnp.concatenate([h1, h1], axis=1), frame_row(0, r))
    load_b.wait()
    load_c.wait()
    for r in range(TILE):
        c0[pl.ds(r * TILE, TILE), :] = ci[r, :, 0:LANES]
        v = ci[r, :, LANES:C_HID]
        c1[pl.ds(r * TILE, TILE), :] = jnp.concatenate([v, v], axis=1)
    for side in range(2):
        ce[side, 0] = c0[pl.ds((TILE - 1) * side, TILE, stride=TILE), :]
        ce[side, 1] = c1[pl.ds((TILE - 1) * side, TILE, stride=TILE), :]
        at = pl.ds(8 + (TILE - 1) * side, TILE, stride=PITCH)
        cs[side, :, 0:LANES] = st0[at, :].astype(BF16)
        cs[side, :, LANES:256] = st1[at, :].astype(BF16)

    def build_row(r, out_slot):
        target = r + 1 if r < TILE else (0 if r == TILE else TILE + 1)
        for dx in range(3):
            v0 = st0[pl.ds(r * PITCH + 7 + dx, TILE), :].astype(BF16)
            v1 = st1[pl.ds(r * PITCH + 7 + dx, TILE), :].astype(BF16)
            if dx != 1 or r not in (0, TILE - 1):
                lhs[dx, target, :, 0:LANES] = v0
                lhs[dx, target, :, LANES:256] = v1
            if dx == 1 and out_slot is not None:
                hidden[out_slot, r, :, 0:LANES] = v0
                hidden[out_slot, r, :, LANES:C_HID] = v1[:, 0:C_IN]

    def cell(gates, c0_prev, c1_prev):
        s0, s1, s2, s3 = (sigmoid(gates[k]) for k in range(4))
        scale = jnp.where(low, 0.5, 1.0)
        t4 = jnp.tanh(gates[4] * scale) * scale + jnp.where(low, 0.5, 0.0)
        t5 = jnp.tanh(gates[5])
        r1, r2, r4, r5 = (pltpu.roll(v, 64, 1) for v in (s1, s2, t4, t5))
        c0_next = jnp.where(low, r1, r2) * c0_prev + s0 * jnp.where(low, r4, r5)
        c1_next = r2 * c1_prev + s1 * r5
        return s3 * jnp.tanh(c0_next), t4 * jnp.tanh(c1_next), c0_next, c1_next

    def bias_piece(k):
        return bb[k * LANES:(k + 1) * LANES].reshape(1, LANES)

    def chunk_gates(rows, halves):
        x = [jnp.concatenate([lhs[dx, r + dy] for r in rows], axis=0) for dy in range(3) for dx in range(3)]
        x = jnp.concatenate(x, axis=1)
        weights = w[...].reshape(9 * 256, 4 * C_HID)
        wide = jnp.dot(x, weights[:, 0:512], preferred_element_type=F32)
        size = x.shape[0] // halves
        rest = [jnp.dot(x[k * size:(k + 1) * size], weights[:, 512:], preferred_element_type=F32) for k in range(halves)]
        return wide, jnp.concatenate(rest, axis=0)

    def gate_row(gates, j, r):
        pre = jnp.concatenate([g[j * TILE:(j + 1) * TILE] for g in gates], axis=1)
        pre = [pre[:, k * LANES:(k + 1) * LANES] + bias_piece(k) for k in range(6)]
        for k in range(6):
            ge[0, k, pl.ds(r * 8, 8), :] = pre[k][0:8]
            ge[1, k, pl.ds(r * 8, 8), :] = pre[k][24:32]
        return pre

    def cell_row(gates, j, r, x_slot):
        pre = gate_row(gates, j, r)
        at = pl.ds(r * TILE, TILE)
        h0, h1, c0_next, c1_next = cell(pre, c0[at, :], c1[at, :])
        c0[at, :] = c0_next
        c1[at, :] = c1_next
        st0[pl.ds(r * PITCH + 8, TILE), :] = h0
        st1[pl.ds(r * PITCH + 8, TILE), :] = jnp.where(low, h1, frame_row(x_slot, r))

    def cell_row_late(j, r, t):
        at = pl.ds(r * TILE, TILE)
        here = pl.ds(r * PITCH + 8, TILE)
        live = jnp.full((TILE, LANES), t, jnp.int32) > 0
        inner = live & (cell_at > 0) & (cell_at < TILE - 1)
        h0, h1, c0_next, c1_next = cell([gp[j, k] for k in range(6)], c0[at, :], c1[at, :])
        c0[at, :] = jnp.where(live, c0_next, c0[at, :])
        c1[at, :] = jnp.where(live, c1_next, c1[at, :])
        st0[here, :] = jnp.where(inner, h0, st0[here, :])
        st1[here, :] = jnp.where(inner & low, h1, st1[here, :])

    def sends(slot):
        pieces = (
            (UP, lhs.at[1, 1], row_in.at[slot, 1]),
            (DOWN, lhs.at[1, TILE], row_in.at[slot, 0]),
            (LEFT, cs.at[0], col_in.at[slot, 1]),
            (RIGHT, cs.at[1], col_in.at[slot, 0]),
            ((-1, -1), cs.at[0, 0:16], diag_in.at[slot, 3]),
            ((-1, 1), cs.at[1, 0:16], diag_in.at[slot, 2]),
            ((1, -1), cs.at[0, 16:32], diag_in.at[slot, 1]),
            ((1, 1), cs.at[1, 16:32], diag_in.at[slot, 0]),
        )
        return [(d, pltpu.make_async_remote_copy(
            src_ref=src, dst_ref=dst, send_sem=send_sem.at[slot, k], recv_sem=recv_sem.at[slot, k],
            device_id=device(d), device_id_type=MESH)) for k, (d, src, dst) in enumerate(pieces)]

    def wait_recv(copies, which):
        for k in which:
            d, copy = copies[k]
            @pl.when(there((-d[0], -d[1])))
            def _():
                copy.wait_recv()

    def step(t, _):
        slot = lax.rem(t, 2)
        x_slot = lax.rem(t + 1, 2)
        copies = sends(slot)

        done = lax.rem(t + STEPS - 1, STEPS)
        for r in (0, TILE - 1):
            here = pl.ds(r * PITCH + 8, TILE)
            lhs[1, r + 1, :, 0:LANES] = st0[here, :].astype(BF16)
            lhs[1, r + 1, :, LANES:256] = st1[here, :].astype(BF16)
        for d, copy in copies:
            @pl.when(there(d))
            def _():
                copy.start()

        @pl.when(t < STEPS - 1)
        def _():
            frame_copy(t + 1, x_slot).wait()

        @pl.when(t == 0)
        def _():
            load_w0.wait()
            load_w1.wait()

        built = 0
        before = None
        for i, rows in enumerate(ROW_SETS[:-1]):
            top = min(max(rows) + 2, TILE)
            for r in range(built, top):
                build_row(r, done)
            built = top
            gates = chunk_gates(rows, HALVES[i])
            if i == 0:
                for j in range(LATE):
                    cell_row_late(j, ROW_SETS[-1][j], t)
            if before is not None:
                for j, r in enumerate(ROW_SETS[i - 1]):
                    cell_row(before, j, r, x_slot)
            before = gates
        for r in range(built, TILE):
            build_row(r, done)

        wait_recv(copies, (0, 1))
        @pl.when(t < STEPS - 2)
        def _():
            frame_copy(t + 2, slot).start()
        for k in range(2):
            at = pl.ds((TILE + k) * PITCH + 8, TILE)
            st0[at, :] = row_in[slot, k, :, 0:LANES].astype(F32)
            st1[at, :] = row_in[slot, k, :, LANES:256].astype(F32)
            build_row(TILE + k, None)
        more = chunk_gates(ROW_SETS[-1], HALVES[-1])
        for j, r in enumerate(ROW_SETS[-2]):
            cell_row(before, j, r, x_slot)

        wait_recv(copies, range(2, 8))
        for d, copy in copies:
            @pl.when(there(d))
            def _():
                copy.wait_send()
        for side in range(2):
            for k in range(2):
                part = slice(k * LANES, (k + 1) * LANES)
                cv[side, k, 8:40, :] = col_in[slot, side, :, part].astype(F32)
                cv[side, k, 7:8, :] = diag_in[slot, side, 15:16, part].astype(F32)
                cv[side, k, 40:41, :] = diag_in[slot, 2 + side, 0:1, part].astype(F32)
        extra = []
        for side in range(2):
            halo = jnp.concatenate([cv[side, k, 7 + dy:39 + dy, :].astype(BF16) for dy in range(3) for k in range(2)], axis=1)
            taps = jnp.concatenate([w[dy * 3 + 2 * side] for dy in range(3)], axis=0)
            extra.append(jnp.dot(halo, taps, preferred_element_type=F32))
        for j, r in enumerate(ROW_SETS[-1]):
            if j < LATE:
                for k, v in enumerate(gate_row(more, j, r)):
                    gp[j, k] = v
                st1[pl.ds(r * PITCH + 8, TILE), :] = frame_row(x_slot, r)
            else:
                cell_row(more, j, r, x_slot)
        for side in range(2):
            more = [extra[side][:, k * LANES:(k + 1) * LANES] for k in range(6)]
            pre = [ge[side, k, pl.ds(7 * side, TILE, stride=8), :] + more[k] for k in range(6)]
            h0, h1, c0_next, c1_next = cell(pre, ce[side, 0], ce[side, 1])
            ce[side, 0] = c0_next
            ce[side, 1] = c1_next
            at = pl.ds(8 + (TILE - 1) * side, TILE, stride=PITCH)
            h1 = jnp.where(low, h1, st1[at, :])
            st0[at, :] = h0
            st1[at, :] = h1
            cs[side, :, 0:LANES] = h0.astype(BF16)
            cs[side, :, LANES:256] = h1.astype(BF16)
        return 0

    lax.fori_loop(0, STEPS, step, 0)

    for j in range(LATE):
        cell_row_late(j, ROW_SETS[-1][j], STEPS)
    for r in range(TILE):
        at = pl.ds(r * PITCH + 8, TILE)
        hidden[STEPS - 1, r, :, 0:LANES] = st0[at, :].astype(BF16)
        hidden[STEPS - 1, r, :, LANES:C_HID] = st1[at, :].astype(BF16)[:, 0:C_IN]
    for side in range(2):
        c0[pl.ds((TILE - 1) * side, TILE, stride=TILE), :] = ce[side, 0]
        c1[pl.ds((TILE - 1) * side, TILE, stride=TILE), :] = ce[side, 1]
    for r in range(TILE):
        at = pl.ds(r * TILE, TILE)
        c_out[r, :, 0:LANES] = c0[at, :]
        c_out[r, :, LANES:C_HID] = c1[at, :][:, 0:C_IN]


def store_kernel(hidden, c_last, hidden_out, c_out, sem):
    copies = [pltpu.make_async_copy(c_last, c_out, sem.at[STEPS])]
    copies += [pltpu.make_async_copy(hidden.at[t], hidden_out.at[t], sem.at[t]) for t in range(STEPS)]
    for copy in copies:
        copy.start()
    for copy in copies:
        copy.wait()


def solution(mesh):
    n_rows = mesh.shape["rows"]
    n_cols = mesh.shape["cols"]
    seq_spec = P(None, "dp", "rows", "cols", None)
    state_spec = P("dp", "rows", "cols", None)

    def local_run(frames, w_in, w_rec, gate_bias, h_init, c_init):
        frames = frames.reshape(STEPS, TILE, TILE, C_IN)
        w_in = w_in.reshape(9, C_IN, 4 * C_HID)
        w_rec = w_rec.reshape(9, C_HID, 4 * C_HID)
        h_init = h_init.reshape(TILE, TILE, C_HID)
        c_init = c_init.reshape(TILE, TILE, C_HID)
        hbm = pl.BlockSpec(memory_space=pltpu.HBM)
        vmem = pl.BlockSpec(memory_space=pltpu.VMEM)
        dma = pltpu.SemaphoreType.DMA
        hidden, c_last = pl.pallas_call(
            functools.partial(kernel, n_rows, n_cols),
            out_shape=(
                pltpu.VMEM((STEPS, TILE, TILE, C_HID), BF16),
                pltpu.VMEM((TILE, TILE, C_HID), F32),
            ),
            in_specs=[hbm] * 6,
            out_specs=(vmem, vmem),
            scratch_shapes=[
                pltpu.VMEM((9, 256, 4 * C_HID), BF16),
                pltpu.VMEM((3, TILE + 2, TILE, 256), BF16),
                pltpu.VMEM(((TILE + 2) * PITCH, LANES), F32),
                pltpu.VMEM(((TILE + 2) * PITCH, LANES), F32),
                pltpu.VMEM((TILE * TILE, LANES), F32),
                pltpu.VMEM((TILE * TILE, LANES), F32),
                pltpu.VMEM((2, 6, 8 * TILE, LANES), F32),
                pltpu.VMEM((LATE, 6, TILE, LANES), F32),
                pltpu.VMEM((2, 2, TILE, LANES), F32),
                pltpu.VMEM((2, 2, PITCH, LANES), F32),
                pltpu.VMEM((2, TILE, TILE, C_IN), BF16),
                pltpu.VMEM((TILE, TILE, C_HID), BF16),
                pltpu.VMEM((4 * C_HID,), F32),
                pltpu.VMEM((TILE, TILE, C_HID), F32),
                pltpu.VMEM((2, TILE, 256), BF16),
                pltpu.VMEM((2, 2, TILE, 256), BF16),
                pltpu.VMEM((2, 2, TILE, 256), BF16),
                pltpu.VMEM((2, 4, 16, 256), BF16),
                dma((2, 8)), dma((2, 8)), dma((2,)), dma((5,)),
            ],
            compiler_params=pltpu.CompilerParams(collective_id=0, has_side_effects=True, vmem_limit_bytes=52 * 1024 * 1024),
        )(frames, w_in, w_rec, gate_bias, h_init, c_init)
        hidden = pltpu.with_memory_space_constraint(hidden, pltpu.VMEM)
        c_last = pltpu.with_memory_space_constraint(c_last, pltpu.VMEM)
        hidden, c_last = pl.pallas_call(
            store_kernel,
            out_shape=(
                jax.ShapeDtypeStruct((STEPS, TILE, TILE, C_HID), BF16),
                jax.ShapeDtypeStruct((TILE, TILE, C_HID), F32),
            ),
            in_specs=[vmem, vmem],
            out_specs=(hbm, hbm),
            scratch_shapes=[dma((STEPS + 1,))],
            compiler_params=pltpu.CompilerParams(vmem_limit_bytes=1024 * 1024),
        )(hidden, c_last)
        return hidden.reshape(STEPS, 1, TILE, TILE, C_HID), c_last.reshape(1, TILE, TILE, C_HID)

    return jax.shard_map(local_run, mesh=mesh, in_specs=(seq_spec, P(), P(), P(), state_spec, state_spec), out_specs=(seq_spec, state_spec), check_vma=False)
```

```python
import functools

import jax
import jax.numpy as jnp
from jax import lax
from jax.experimental import pallas as pl
from jax.experimental.pallas import tpu as pltpu
from jax.sharding import PartitionSpec as P

MESH = pl.DeviceIdType.MESH
F32, BF16 = jnp.float32, jnp.bfloat16

STEPS = 16
TILE = 32
C_IN, C_HID = 64, 192
LANES = 128
PITCH = 48
ROW_SETS = (range(1, 9), range(9, 17), range(17, 25), (*range(25, 31), 0, 31))
HALVES = (2, 2, 2, 2)
SPLIT3 = 8
SPLIT4 = 8
LATE = 6

UP, DOWN, LEFT, RIGHT = (-1, 0), (1, 0), (0, -1), (0, 1)
DIRS = (UP, DOWN, LEFT, RIGHT, (-1, -1), (-1, 1), (1, -1), (1, 1))


def sigmoid(x):
    return 0.5 * jnp.tanh(0.5 * x) + 0.5


def kernel(n_rows, n_cols, frames, w_in, w_rec, bias, h_init, c_init, hidden, c_out,
         w, lhs, st0, st1, c0, c1, ge, gp, ce, cv, fb, hb, bb, ci, cs, row_in, col_in, diag_in,
         send_sem, recv_sem, frame_sem, load_sem):
    my_row, my_col = lax.axis_index("rows"), lax.axis_index("cols")

    def there(d):
        r, c = my_row + d[0], my_col + d[1]
        return (r >= 0) & (r < n_rows) & (c >= 0) & (c < n_cols)

    def device(d):
        return {"rows": my_row + d[0], "cols": my_col + d[1]}

    load_w0 = pltpu.make_async_copy(w_rec, w.at[:, 0:C_HID, :], load_sem.at[0])
    load_w1 = pltpu.make_async_copy(w_in, w.at[:, C_HID:256, :], load_sem.at[1])
    load_h = pltpu.make_async_copy(h_init, hb, load_sem.at[2])
    load_c = pltpu.make_async_copy(c_init, ci, load_sem.at[3])

    def frame_copy(t, slot):
        return pltpu.make_async_copy(frames.at[t], fb.at[slot], frame_sem.at[slot])

    load_b = pltpu.make_async_copy(bias, bb, load_sem.at[4])
    load_h.start()
    load_b.start()
    frame_copy(0, 0).start()
    load_c.start()
    load_w0.start()
    load_w1.start()
    frame_copy(1, 1).start()

    row_in[...] = jnp.zeros_like(row_in)
    col_in[...] = jnp.zeros_like(col_in)
    diag_in[...] = jnp.zeros_like(diag_in)
    gp[...] = jnp.zeros_like(gp)
    for k in range(TILE + 2):
        for st in (st0, st1):
            st[pl.ds(k * PITCH, 8), :] = jnp.zeros((8, LANES), F32)
            st[pl.ds(k * PITCH + 40, 8), :] = jnp.zeros((8, LANES), F32)

    barrier = pltpu.get_barrier_semaphore()
    for d in DIRS:
        @pl.when(there(d))
        def _():
            pl.semaphore_signal(barrier, inc=1, device_id=device(d), device_id_type=MESH)
    def near(i, n):
        return 1 + (i > 0).astype(jnp.int32) + (i < n - 1).astype(jnp.int32)

    pl.semaphore_wait(barrier, near(my_row, n_rows) * near(my_col, n_cols) - 1)

    lane = lax.broadcasted_iota(jnp.int32, (TILE, LANES), 1)
    low = lane < C_IN
    cell_at = lax.broadcasted_iota(jnp.int32, (TILE, LANES), 0)

    def frame_row(slot, r):
        x = fb[slot, r].astype(F32)
        return jnp.concatenate([x, x], axis=1)

    load_h.wait()
    frame_copy(0, 0).wait()
    for r in range(TILE):
        st0[pl.ds(r * PITCH + 8, TILE), :] = hb[r, :, 0:LANES].astype(F32)
        h1 = hb[r, :, LANES:C_HID].astype(F32)
        st1[pl.ds(r * PITCH + 8, TILE), :] = jnp.where(low, jnp.concatenate([h1, h1], axis=1), frame_row(0, r))
    load_b.wait()
    load_c.wait()
    for r in range(TILE):
        c0[pl.ds(r * TILE, TILE), :] = ci[r, :, 0:LANES]
        v = ci[r, :, LANES:C_HID]
        c1[pl.ds(r * TILE, TILE), :] = jnp.concatenate([v, v], axis=1)
    for side in range(2):
        ce[side, 0] = c0[pl.ds((TILE - 1) * side, TILE, stride=TILE), :]
        ce[side, 1] = c1[pl.ds((TILE - 1) * side, TILE, stride=TILE), :]
        at = pl.ds(8 + (TILE - 1) * side, TILE, stride=PITCH)
        cs[side, :, 0:LANES] = st0[at, :].astype(BF16)
        cs[side, :, LANES:256] = st1[at, :].astype(BF16)

    def build_row(r, out_slot):
        target = r + 1 if r < TILE else (0 if r == TILE else TILE + 1)
        for dx in range(3):
            v0 = st0[pl.ds(r * PITCH + 7 + dx, TILE), :].astype(BF16)
            v1 = st1[pl.ds(r * PITCH + 7 + dx, TILE), :].astype(BF16)
            if dx != 1 or r not in (0, TILE - 1):
                lhs[dx, target, :, 0:LANES] = v0
                lhs[dx, target, :, LANES:256] = v1
            if dx == 1 and out_slot is not None:
                hidden[out_slot, r, :, 0:LANES] = v0
                hidden[out_slot, r, :, LANES:C_HID] = v1[:, 0:C_IN]

    def cell(gates, c0_prev, c1_prev):
        s0, s1, s2, s3 = (sigmoid(gates[k]) for k in range(4))
        scale = jnp.where(low, 0.5, 1.0)
        t4 = jnp.tanh(gates[4] * scale) * scale + jnp.where(low, 0.5, 0.0)
        t5 = jnp.tanh(gates[5])
        r1, r2, r4, r5 = (pltpu.roll(v, 64, 1) for v in (s1, s2, t4, t5))
        c0_next = jnp.where(low, r1, r2) * c0_prev + s0 * jnp.where(low, r4, r5)
        c1_next = r2 * c1_prev + s1 * r5
        return s3 * jnp.tanh(c0_next), t4 * jnp.tanh(c1_next), c0_next, c1_next

    def bias_piece(k):
        return bb[k * LANES:(k + 1) * LANES].reshape(1, LANES)

    def products(rows, halves, taps):
        x = [jnp.concatenate([lhs[tap % 3, r + tap // 3] for r in rows], axis=0) for tap in taps]
        x = jnp.concatenate(x, axis=1)
        weights = w[taps[0]:taps[-1] + 1].reshape(len(taps) * 256, 4 * C_HID)
        size = x.shape[0] // halves
        rest = [jnp.dot(x[k * size:(k + 1) * size], weights[:, 512:], preferred_element_type=F32) for k in range(halves)]
        return [jnp.dot(x, weights[:, 0:512], preferred_element_type=F32)] + rest

    def whole(parts):
        return parts[0], jnp.concatenate(parts[1:], axis=0)

    def chunk_gates(rows, halves):
        return whole(products(rows, halves, range(9)))

    def gate_row(gates, j, r):
        pre = jnp.concatenate([g[j * TILE:(j + 1) * TILE] for g in gates], axis=1)
        pre = [pre[:, k * LANES:(k + 1) * LANES] + bias_piece(k) for k in range(6)]
        for k in range(6):
            ge[0, k, pl.ds(r * 8, 8), :] = pre[k][0:8]
            ge[1, k, pl.ds(r * 8, 8), :] = pre[k][24:32]
        return pre

    def cell_row(gates, j, r, x_slot):
        pre = gate_row(gates, j, r)
        at = pl.ds(r * TILE, TILE)
        h0, h1, c0_next, c1_next = cell(pre, c0[at, :], c1[at, :])
        c0[at, :] = c0_next
        c1[at, :] = c1_next
        st0[pl.ds(r * PITCH + 8, TILE), :] = h0
        st1[pl.ds(r * PITCH + 8, TILE), :] = jnp.where(low, h1, frame_row(x_slot, r))

    def cell_row_late(j, r, t):
        at = pl.ds(r * TILE, TILE)
        here = pl.ds(r * PITCH + 8, TILE)
        live = jnp.full((TILE, LANES), t, jnp.int32) > 0
        inner = live & (cell_at > 0) & (cell_at < TILE - 1)
        h0, h1, c0_next, c1_next = cell([gp[j, k] for k in range(6)], c0[at, :], c1[at, :])
        c0[at, :] = jnp.where(live, c0_next, c0[at, :])
        c1[at, :] = jnp.where(live, c1_next, c1[at, :])
        st0[here, :] = jnp.where(inner, h0, st0[here, :])
        st1[here, :] = jnp.where(inner & low, h1, st1[here, :])

    def sends(slot):
        pieces = (
            (UP, lhs.at[1, 1], row_in.at[slot, 1]),
            (DOWN, lhs.at[1, TILE], row_in.at[slot, 0]),
            (LEFT, cs.at[0], col_in.at[slot, 1]),
            (RIGHT, cs.at[1], col_in.at[slot, 0]),
            ((-1, -1), cs.at[0, 0:16], diag_in.at[slot, 3]),
            ((-1, 1), cs.at[1, 0:16], diag_in.at[slot, 2]),
            ((1, -1), cs.at[0, 16:32], diag_in.at[slot, 1]),
            ((1, 1), cs.at[1, 16:32], diag_in.at[slot, 0]),
        )
        return [(d, pltpu.make_async_remote_copy(
            src_ref=src, dst_ref=dst, send_sem=send_sem.at[slot, k], recv_sem=recv_sem.at[slot, k],
            device_id=device(d), device_id_type=MESH)) for k, (d, src, dst) in enumerate(pieces)]

    def wait_recv(copies, which):
        for k in which:
            d, copy = copies[k]
            @pl.when(there((-d[0], -d[1])))
            def _():
                copy.wait_recv()

    def step(t, _):
        slot = lax.rem(t, 2)
        x_slot = lax.rem(t + 1, 2)
        copies = sends(slot)

        done = lax.rem(t + STEPS - 1, STEPS)
        for r in (0, TILE - 1):
            here = pl.ds(r * PITCH + 8, TILE)
            lhs[1, r + 1, :, 0:LANES] = st0[here, :].astype(BF16)
            lhs[1, r + 1, :, LANES:256] = st1[here, :].astype(BF16)
        for d, copy in copies:
            @pl.when(there(d))
            def _():
                copy.start()

        @pl.when(t < STEPS - 2)
        def _():
            frame_copy(t + 2, slot).start()
        @pl.when(t < STEPS - 1)
        def _():
            frame_copy(t + 1, x_slot).wait()

        @pl.when(t == 0)
        def _():
            load_w0.wait()
            load_w1.wait()

        built = 0
        before = None
        for i, rows in enumerate(ROW_SETS[:-1]):
            top = min(max(rows) + 2, TILE)
            for r in range(built, top):
                build_row(r, done)
            built = top
            if i < len(ROW_SETS) - 2:
                gates = chunk_gates(rows, HALVES[i])
            else:
                gates = products(rows, HALVES[i], range(SPLIT3))
            if i == 0:
                for j in range(LATE):
                    cell_row_late(j, ROW_SETS[-1][j], t)
            if before is not None:
                for j, r in enumerate(ROW_SETS[i - 1]):
                    cell_row(before, j, r, x_slot)
            before = gates
        for r in range(built, TILE):
            build_row(r, done)

        wait_recv(copies, (0, 1))
        rest = products(ROW_SETS[-2], HALVES[-2], range(SPLIT3, 9))
        before = whole([b + a for a, b in zip(before, rest)])
        for k in range(2):
            at = pl.ds((TILE + k) * PITCH + 8, TILE)
            st0[at, :] = row_in[slot, k, :, 0:LANES].astype(F32)
            st1[at, :] = row_in[slot, k, :, LANES:256].astype(F32)
            build_row(TILE + k, None)
        more = products(ROW_SETS[-1], HALVES[-1], range(SPLIT4))
        for j, r in enumerate(ROW_SETS[-2]):
            cell_row(before, j, r, x_slot)

        wait_recv(copies, range(2, 8))
        for d, copy in copies:
            @pl.when(there(d))
            def _():
                copy.wait_send()
        rest = products(ROW_SETS[-1], HALVES[-1], range(SPLIT4, 9))
        more = whole([b + a for a, b in zip(more, rest)])
        for side in range(2):
            for k in range(2):
                part = slice(k * LANES, (k + 1) * LANES)
                cv[side, k, 8:40, :] = col_in[slot, side, :, part].astype(F32)
                cv[side, k, 7:8, :] = diag_in[slot, side, 15:16, part].astype(F32)
                cv[side, k, 40:41, :] = diag_in[slot, 2 + side, 0:1, part].astype(F32)
        extra = []
        for side in range(2):
            halo = jnp.concatenate([cv[side, k, 7 + dy:39 + dy, :].astype(BF16) for dy in range(3) for k in range(2)], axis=1)
            taps = jnp.concatenate([w[dy * 3 + 2 * side] for dy in range(3)], axis=0)
            extra.append(jnp.dot(halo, taps, preferred_element_type=F32))
        for j, r in enumerate(ROW_SETS[-1]):
            if j < LATE:
                for k, v in enumerate(gate_row(more, j, r)):
                    gp[j, k] = v
                st1[pl.ds(r * PITCH + 8, TILE), :] = frame_row(x_slot, r)
            else:
                cell_row(more, j, r, x_slot)
        for side in range(2):
            more = [extra[side][:, k * LANES:(k + 1) * LANES] for k in range(6)]
            pre = [ge[side, k, pl.ds(7 * side, TILE, stride=8), :] + more[k] for k in range(6)]
            h0, h1, c0_next, c1_next = cell(pre, ce[side, 0], ce[side, 1])
            ce[side, 0] = c0_next
            ce[side, 1] = c1_next
            at = pl.ds(8 + (TILE - 1) * side, TILE, stride=PITCH)
            h1 = jnp.where(low, h1, st1[at, :])
            st0[at, :] = h0
            st1[at, :] = h1
            cs[side, :, 0:LANES] = h0.astype(BF16)
            cs[side, :, LANES:256] = h1.astype(BF16)
        return 0

    lax.fori_loop(0, STEPS, step, 0)

    for j in range(LATE):
        cell_row_late(j, ROW_SETS[-1][j], STEPS)
    for r in range(TILE):
        at = pl.ds(r * PITCH + 8, TILE)
        hidden[STEPS - 1, r, :, 0:LANES] = st0[at, :].astype(BF16)
        hidden[STEPS - 1, r, :, LANES:C_HID] = st1[at, :].astype(BF16)[:, 0:C_IN]
    for side in range(2):
        c0[pl.ds((TILE - 1) * side, TILE, stride=TILE), :] = ce[side, 0]
        c1[pl.ds((TILE - 1) * side, TILE, stride=TILE), :] = ce[side, 1]
    for r in range(TILE):
        at = pl.ds(r * TILE, TILE)
        c_out[r, :, 0:LANES] = c0[at, :]
        c_out[r, :, LANES:C_HID] = c1[at, :][:, 0:C_IN]


def store_kernel(hidden, c_last, hidden_out, c_out, sem):
    copies = [pltpu.make_async_copy(c_last, c_out, sem.at[STEPS])]
    copies += [pltpu.make_async_copy(hidden.at[t], hidden_out.at[t], sem.at[t]) for t in range(STEPS)]
    for copy in copies:
        copy.start()
    for copy in copies:
        copy.wait()


def solution(mesh):
    n_rows = mesh.shape["rows"]
    n_cols = mesh.shape["cols"]
    seq_spec = P(None, "dp", "rows", "cols", None)
    state_spec = P("dp", "rows", "cols", None)

    def local_run(frames, w_in, w_rec, gate_bias, h_init, c_init):
        frames = frames.reshape(STEPS, TILE, TILE, C_IN)
        w_in = w_in.reshape(9, C_IN, 4 * C_HID)
        w_rec = w_rec.reshape(9, C_HID, 4 * C_HID)
        h_init = h_init.reshape(TILE, TILE, C_HID)
        c_init = c_init.reshape(TILE, TILE, C_HID)
        hbm = pl.BlockSpec(memory_space=pltpu.HBM)
        vmem = pl.BlockSpec(memory_space=pltpu.VMEM)
        dma = pltpu.SemaphoreType.DMA
        hidden, c_last = pl.pallas_call(
            functools.partial(kernel, n_rows, n_cols),
            out_shape=(
                pltpu.VMEM((STEPS, TILE, TILE, C_HID), BF16),
                pltpu.VMEM((TILE, TILE, C_HID), F32),
            ),
            in_specs=[hbm] * 6,
            out_specs=(vmem, vmem),
            scratch_shapes=[
                pltpu.VMEM((9, 256, 4 * C_HID), BF16),
                pltpu.VMEM((3, TILE + 2, TILE, 256), BF16),
                pltpu.VMEM(((TILE + 2) * PITCH, LANES), F32),
                pltpu.VMEM(((TILE + 2) * PITCH, LANES), F32),
                pltpu.VMEM((TILE * TILE, LANES), F32),
                pltpu.VMEM((TILE * TILE, LANES), F32),
                pltpu.VMEM((2, 6, 8 * TILE, LANES), F32),
                pltpu.VMEM((LATE, 6, TILE, LANES), F32),
                pltpu.VMEM((2, 2, TILE, LANES), F32),
                pltpu.VMEM((2, 2, PITCH, LANES), F32),
                pltpu.VMEM((2, TILE, TILE, C_IN), BF16),
                pltpu.VMEM((TILE, TILE, C_HID), BF16),
                pltpu.VMEM((4 * C_HID,), F32),
                pltpu.VMEM((TILE, TILE, C_HID), F32),
                pltpu.VMEM((2, TILE, 256), BF16),
                pltpu.VMEM((2, 2, TILE, 256), BF16),
                pltpu.VMEM((2, 2, TILE, 256), BF16),
                pltpu.VMEM((2, 4, 16, 256), BF16),
                dma((2, 8)), dma((2, 8)), dma((2,)), dma((5,)),
            ],
            compiler_params=pltpu.CompilerParams(collective_id=0, has_side_effects=True, vmem_limit_bytes=52 * 1024 * 1024),
        )(frames, w_in, w_rec, gate_bias, h_init, c_init)
        hidden = pltpu.with_memory_space_constraint(hidden, pltpu.VMEM)
        c_last = pltpu.with_memory_space_constraint(c_last, pltpu.VMEM)
        hidden, c_last = pl.pallas_call(
            store_kernel,
            out_shape=(
                jax.ShapeDtypeStruct((STEPS, TILE, TILE, C_HID), BF16),
                jax.ShapeDtypeStruct((TILE, TILE, C_HID), F32),
            ),
            in_specs=[vmem, vmem],
            out_specs=(hbm, hbm),
            scratch_shapes=[dma((STEPS + 1,))],
            compiler_params=pltpu.CompilerParams(vmem_limit_bytes=1024 * 1024),
        )(hidden, c_last)
        return hidden.reshape(STEPS, 1, TILE, TILE, C_HID), c_last.reshape(1, TILE, TILE, C_HID)

    return jax.shard_map(local_run, mesh=mesh, in_specs=(seq_spec, P(), P(), P(), state_spec, state_spec), out_specs=(seq_spec, state_spec), check_vma=False)
```

```python
import functools

import jax
import jax.numpy as jnp
from jax import lax
from jax.experimental import pallas as pl
from jax.experimental.pallas import tpu as pltpu
from jax.sharding import PartitionSpec as P

MESH = pl.DeviceIdType.MESH
F32, BF16 = jnp.float32, jnp.bfloat16

STEPS = 16
TILE = 32
C_IN, C_HID = 64, 192
LANES = 128
PITCH = 48
ROW_SETS = (range(1, 9), range(9, 17), range(17, 25), (*range(25, 31), 0, 31))
HALVES = (1, 1, 2, 2)
SPLIT3 = 8
SPLIT4 = 8
LATE = 6

UP, DOWN, LEFT, RIGHT = (-1, 0), (1, 0), (0, -1), (0, 1)
DIRS = (UP, DOWN, LEFT, RIGHT, (-1, -1), (-1, 1), (1, -1), (1, 1))


def sigmoid(x):
    return 0.5 * jnp.tanh(0.5 * x) + 0.5


def kernel(n_rows, n_cols, frames, w_in, w_rec, bias, h_init, c_init, hidden, c_out,
         w, lhs, st0, st1, c0, c1, ge, gp, ce, cv, fb, hb, bb, ci, cs, row_in, col_in, diag_in,
         send_sem, recv_sem, frame_sem, load_sem):
    my_row, my_col = lax.axis_index("rows"), lax.axis_index("cols")

    def there(d):
        r, c = my_row + d[0], my_col + d[1]
        return (r >= 0) & (r < n_rows) & (c >= 0) & (c < n_cols)

    def device(d):
        return {"rows": my_row + d[0], "cols": my_col + d[1]}

    load_w0 = pltpu.make_async_copy(w_rec, w.at[:, 0:C_HID, :], load_sem.at[0])
    load_w1 = pltpu.make_async_copy(w_in, w.at[:, C_HID:256, :], load_sem.at[1])
    load_h = pltpu.make_async_copy(h_init, hb, load_sem.at[2])
    load_c = pltpu.make_async_copy(c_init, ci, load_sem.at[3])

    def frame_copy(t, slot):
        return pltpu.make_async_copy(frames.at[t], fb.at[slot], frame_sem.at[slot])

    load_b = pltpu.make_async_copy(bias, bb, load_sem.at[4])
    load_h.start()
    load_b.start()
    frame_copy(0, 0).start()
    load_c.start()
    load_w0.start()
    load_w1.start()
    frame_copy(1, 1).start()

    row_in[...] = jnp.zeros_like(row_in)
    col_in[...] = jnp.zeros_like(col_in)
    diag_in[...] = jnp.zeros_like(diag_in)
    gp[...] = jnp.zeros_like(gp)
    for k in range(TILE + 2):
        for st in (st0, st1):
            st[pl.ds(k * PITCH, 8), :] = jnp.zeros((8, LANES), F32)
            st[pl.ds(k * PITCH + 40, 8), :] = jnp.zeros((8, LANES), F32)

    barrier = pltpu.get_barrier_semaphore()
    for d in DIRS:
        @pl.when(there(d))
        def _():
            pl.semaphore_signal(barrier, inc=1, device_id=device(d), device_id_type=MESH)
    def near(i, n):
        return 1 + (i > 0).astype(jnp.int32) + (i < n - 1).astype(jnp.int32)

    pl.semaphore_wait(barrier, near(my_row, n_rows) * near(my_col, n_cols) - 1)

    lane = lax.broadcasted_iota(jnp.int32, (TILE, LANES), 1)
    low = lane < C_IN
    cell_at = lax.broadcasted_iota(jnp.int32, (TILE, LANES), 0)

    def frame_row(slot, r):
        x = fb[slot, r].astype(F32)
        return jnp.concatenate([x, x], axis=1)

    load_h.wait()
    frame_copy(0, 0).wait()
    for r in range(TILE):
        st0[pl.ds(r * PITCH + 8, TILE), :] = hb[r, :, 0:LANES].astype(F32)
        h1 = hb[r, :, LANES:C_HID].astype(F32)
        st1[pl.ds(r * PITCH + 8, TILE), :] = jnp.where(low, jnp.concatenate([h1, h1], axis=1), frame_row(0, r))
    load_b.wait()
    load_c.wait()
    for r in range(TILE):
        c0[pl.ds(r * TILE, TILE), :] = ci[r, :, 0:LANES]
        v = ci[r, :, LANES:C_HID]
        c1[pl.ds(r * TILE, TILE), :] = jnp.concatenate([v, v], axis=1)
    for side in range(2):
        ce[side, 0] = c0[pl.ds((TILE - 1) * side, TILE, stride=TILE), :]
        ce[side, 1] = c1[pl.ds((TILE - 1) * side, TILE, stride=TILE), :]
        at = pl.ds(8 + (TILE - 1) * side, TILE, stride=PITCH)
        cs[side, :, 0:LANES] = st0[at, :].astype(BF16)
        cs[side, :, LANES:256] = st1[at, :].astype(BF16)

    def build_row(r, out_slot):
        target = r + 1 if r < TILE else (0 if r == TILE else TILE + 1)
        for dx in range(3):
            v0 = st0[pl.ds(r * PITCH + 7 + dx, TILE), :].astype(BF16)
            v1 = st1[pl.ds(r * PITCH + 7 + dx, TILE), :].astype(BF16)
            if dx != 1 or r not in (0, TILE - 1):
                lhs[dx, target, :, 0:LANES] = v0
                lhs[dx, target, :, LANES:256] = v1
            if dx == 1 and out_slot is not None:
                hidden[out_slot, r, :, 0:LANES] = v0
                hidden[out_slot, r, :, LANES:C_HID] = v1[:, 0:C_IN]

    def cell(gates, c0_prev, c1_prev):
        s0, s1, s2, s3 = (sigmoid(gates[k]) for k in range(4))
        scale = jnp.where(low, 0.5, 1.0)
        t4 = jnp.tanh(gates[4] * scale) * scale + jnp.where(low, 0.5, 0.0)
        t5 = jnp.tanh(gates[5])
        r1, r2, r4, r5 = (pltpu.roll(v, 64, 1) for v in (s1, s2, t4, t5))
        c0_next = jnp.where(low, r1, r2) * c0_prev + s0 * jnp.where(low, r4, r5)
        c1_next = r2 * c1_prev + s1 * r5
        return s3 * jnp.tanh(c0_next), t4 * jnp.tanh(c1_next), c0_next, c1_next

    def bias_piece(k):
        return bb[k * LANES:(k + 1) * LANES].reshape(1, LANES)

    def products(rows, halves, taps):
        x = [jnp.concatenate([lhs[tap % 3, r + tap // 3] for r in rows], axis=0) for tap in taps]
        x = jnp.concatenate(x, axis=1)
        weights = w[taps[0]:taps[-1] + 1].reshape(len(taps) * 256, 4 * C_HID)
        size = x.shape[0] // halves
        rest = [jnp.dot(x[k * size:(k + 1) * size], weights[:, 512:], preferred_element_type=F32) for k in range(halves)]
        return [jnp.dot(x, weights[:, 0:512], preferred_element_type=F32)] + rest

    def whole(parts):
        return parts[0], jnp.concatenate(parts[1:], axis=0)

    def chunk_gates(rows, halves):
        return whole(products(rows, halves, range(9)))

    def gate_row(gates, j, r):
        pre = jnp.concatenate([g[j * TILE:(j + 1) * TILE] for g in gates], axis=1)
        pre = [pre[:, k * LANES:(k + 1) * LANES] + bias_piece(k) for k in range(6)]
        for k in range(6):
            ge[0, k, pl.ds(r * 8, 8), :] = pre[k][0:8]
            ge[1, k, pl.ds(r * 8, 8), :] = pre[k][24:32]
        return pre

    def cell_row(gates, j, r, x_slot):
        pre = gate_row(gates, j, r)
        at = pl.ds(r * TILE, TILE)
        h0, h1, c0_next, c1_next = cell(pre, c0[at, :], c1[at, :])
        c0[at, :] = c0_next
        c1[at, :] = c1_next
        st0[pl.ds(r * PITCH + 8, TILE), :] = h0
        st1[pl.ds(r * PITCH + 8, TILE), :] = jnp.where(low, h1, frame_row(x_slot, r))

    def cell_row_late(j, r, t):
        at = pl.ds(r * TILE, TILE)
        here = pl.ds(r * PITCH + 8, TILE)
        live = jnp.full((TILE, LANES), t, jnp.int32) > 0
        inner = live & (cell_at > 0) & (cell_at < TILE - 1)
        h0, h1, c0_next, c1_next = cell([gp[j, k] for k in range(6)], c0[at, :], c1[at, :])
        c0[at, :] = jnp.where(live, c0_next, c0[at, :])
        c1[at, :] = jnp.where(live, c1_next, c1[at, :])
        st0[here, :] = jnp.where(inner, h0, st0[here, :])
        st1[here, :] = jnp.where(inner & low, h1, st1[here, :])

    def sends(slot):
        pieces = (
            (UP, lhs.at[1, 1], row_in.at[slot, 1]),
            (DOWN, lhs.at[1, TILE], row_in.at[slot, 0]),
            (LEFT, cs.at[0], col_in.at[slot, 1]),
            (RIGHT, cs.at[1], col_in.at[slot, 0]),
            ((-1, -1), cs.at[0, 0:16], diag_in.at[slot, 3]),
            ((-1, 1), cs.at[1, 0:16], diag_in.at[slot, 2]),
            ((1, -1), cs.at[0, 16:32], diag_in.at[slot, 1]),
            ((1, 1), cs.at[1, 16:32], diag_in.at[slot, 0]),
        )
        return [(d, pltpu.make_async_remote_copy(
            src_ref=src, dst_ref=dst, send_sem=send_sem.at[slot, k], recv_sem=recv_sem.at[slot, k],
            device_id=device(d), device_id_type=MESH)) for k, (d, src, dst) in enumerate(pieces)]

    def wait_recv(copies, which):
        for k in which:
            d, copy = copies[k]
            @pl.when(there((-d[0], -d[1])))
            def _():
                copy.wait_recv()

    def step(t, _):
        slot = lax.rem(t, 2)
        x_slot = lax.rem(t + 1, 2)
        copies = sends(slot)

        done = lax.rem(t + STEPS - 1, STEPS)
        for r in (0, TILE - 1):
            here = pl.ds(r * PITCH + 8, TILE)
            lhs[1, r + 1, :, 0:LANES] = st0[here, :].astype(BF16)
            lhs[1, r + 1, :, LANES:256] = st1[here, :].astype(BF16)
        for d, copy in copies:
            @pl.when(there(d))
            def _():
                copy.start()

        @pl.when(t < STEPS - 2)
        def _():
            frame_copy(t + 2, slot).start()
        @pl.when(t < STEPS - 1)
        def _():
            frame_copy(t + 1, x_slot).wait()

        @pl.when(t == 0)
        def _():
            load_w0.wait()
            load_w1.wait()

        built = 0
        before = None
        for i, rows in enumerate(ROW_SETS[:-1]):
            top = min(max(rows) + 2, TILE)
            for r in range(built, top):
                build_row(r, done)
            built = top
            if i < len(ROW_SETS) - 2:
                gates = chunk_gates(rows, HALVES[i])
            else:
                gates = products(rows, HALVES[i], range(SPLIT3))
            if i == 0:
                for j in range(LATE):
                    cell_row_late(j, ROW_SETS[-1][j], t)
            if before is not None:
                for j, r in enumerate(ROW_SETS[i - 1]):
                    cell_row(before, j, r, x_slot)
            before = gates
        for r in range(built, TILE):
            build_row(r, done)

        wait_recv(copies, (0, 1))
        rest = products(ROW_SETS[-2], HALVES[-2], range(SPLIT3, 9))
        before = whole([b + a for a, b in zip(before, rest)])
        for k in range(2):
            at = pl.ds((TILE + k) * PITCH + 8, TILE)
            st0[at, :] = row_in[slot, k, :, 0:LANES].astype(F32)
            st1[at, :] = row_in[slot, k, :, LANES:256].astype(F32)
            build_row(TILE + k, None)
        more = products(ROW_SETS[-1], HALVES[-1], range(SPLIT4))
        for j, r in enumerate(ROW_SETS[-2]):
            cell_row(before, j, r, x_slot)

        wait_recv(copies, range(2, 8))
        for d, copy in copies:
            @pl.when(there(d))
            def _():
                copy.wait_send()
        rest = products(ROW_SETS[-1], HALVES[-1], range(SPLIT4, 9))
        more = whole([b + a for a, b in zip(more, rest)])
        for side in range(2):
            for k in range(2):
                part = slice(k * LANES, (k + 1) * LANES)
                cv[side, k, 8:40, :] = col_in[slot, side, :, part].astype(F32)
                cv[side, k, 7:8, :] = diag_in[slot, side, 15:16, part].astype(F32)
                cv[side, k, 40:41, :] = diag_in[slot, 2 + side, 0:1, part].astype(F32)
        extra = []
        for side in range(2):
            halo = jnp.concatenate([cv[side, k, 7 + dy:39 + dy, :].astype(BF16) for dy in range(3) for k in range(2)], axis=1)
            taps = jnp.concatenate([w[dy * 3 + 2 * side] for dy in range(3)], axis=0)
            extra.append(jnp.dot(halo, taps, preferred_element_type=F32))
        for j, r in enumerate(ROW_SETS[-1]):
            if j < LATE:
                for k, v in enumerate(gate_row(more, j, r)):
                    gp[j, k] = v
                st1[pl.ds(r * PITCH + 8, TILE), :] = frame_row(x_slot, r)
            else:
                cell_row(more, j, r, x_slot)
        for side in range(2):
            more = [extra[side][:, k * LANES:(k + 1) * LANES] for k in range(6)]
            pre = [ge[side, k, pl.ds(7 * side, TILE, stride=8), :] + more[k] for k in range(6)]
            h0, h1, c0_next, c1_next = cell(pre, ce[side, 0], ce[side, 1])
            ce[side, 0] = c0_next
            ce[side, 1] = c1_next
            at = pl.ds(8 + (TILE - 1) * side, TILE, stride=PITCH)
            h1 = jnp.where(low, h1, st1[at, :])
            st0[at, :] = h0
            st1[at, :] = h1
            cs[side, :, 0:LANES] = h0.astype(BF16)
            cs[side, :, LANES:256] = h1.astype(BF16)
        return 0

    lax.fori_loop(0, STEPS, step, 0)

    for j in range(LATE):
        cell_row_late(j, ROW_SETS[-1][j], STEPS)
    for r in range(TILE):
        at = pl.ds(r * PITCH + 8, TILE)
        hidden[STEPS - 1, r, :, 0:LANES] = st0[at, :].astype(BF16)
        hidden[STEPS - 1, r, :, LANES:C_HID] = st1[at, :].astype(BF16)[:, 0:C_IN]
    for side in range(2):
        c0[pl.ds((TILE - 1) * side, TILE, stride=TILE), :] = ce[side, 0]
        c1[pl.ds((TILE - 1) * side, TILE, stride=TILE), :] = ce[side, 1]
    for r in range(TILE):
        at = pl.ds(r * TILE, TILE)
        c_out[r, :, 0:LANES] = c0[at, :]
        c_out[r, :, LANES:C_HID] = c1[at, :][:, 0:C_IN]


def store_kernel(hidden, c_last, hidden_out, c_out, sem):
    copies = [pltpu.make_async_copy(c_last, c_out, sem.at[STEPS])]
    copies += [pltpu.make_async_copy(hidden.at[t], hidden_out.at[t], sem.at[t]) for t in range(STEPS)]
    for copy in copies:
        copy.start()
    for copy in copies:
        copy.wait()


def solution(mesh):
    n_rows = mesh.shape["rows"]
    n_cols = mesh.shape["cols"]
    seq_spec = P(None, "dp", "rows", "cols", None)
    state_spec = P("dp", "rows", "cols", None)

    def local_run(frames, w_in, w_rec, gate_bias, h_init, c_init):
        frames = frames.reshape(STEPS, TILE, TILE, C_IN)
        w_in = w_in.reshape(9, C_IN, 4 * C_HID)
        w_rec = w_rec.reshape(9, C_HID, 4 * C_HID)
        h_init = h_init.reshape(TILE, TILE, C_HID)
        c_init = c_init.reshape(TILE, TILE, C_HID)
        hbm = pl.BlockSpec(memory_space=pltpu.HBM)
        vmem = pl.BlockSpec(memory_space=pltpu.VMEM)
        dma = pltpu.SemaphoreType.DMA
        hidden, c_last = pl.pallas_call(
            functools.partial(kernel, n_rows, n_cols),
            out_shape=(
                pltpu.VMEM((STEPS, TILE, TILE, C_HID), BF16),
                pltpu.VMEM((TILE, TILE, C_HID), F32),
            ),
            in_specs=[hbm] * 6,
            out_specs=(vmem, vmem),
            scratch_shapes=[
                pltpu.VMEM((9, 256, 4 * C_HID), BF16),
                pltpu.VMEM((3, TILE + 2, TILE, 256), BF16),
                pltpu.VMEM(((TILE + 2) * PITCH, LANES), F32),
                pltpu.VMEM(((TILE + 2) * PITCH, LANES), F32),
                pltpu.VMEM((TILE * TILE, LANES), F32),
                pltpu.VMEM((TILE * TILE, LANES), F32),
                pltpu.VMEM((2, 6, 8 * TILE, LANES), F32),
                pltpu.VMEM((LATE, 6, TILE, LANES), F32),
                pltpu.VMEM((2, 2, TILE, LANES), F32),
                pltpu.VMEM((2, 2, PITCH, LANES), F32),
                pltpu.VMEM((2, TILE, TILE, C_IN), BF16),
                pltpu.VMEM((TILE, TILE, C_HID), BF16),
                pltpu.VMEM((4 * C_HID,), F32),
                pltpu.VMEM((TILE, TILE, C_HID), F32),
                pltpu.VMEM((2, TILE, 256), BF16),
                pltpu.VMEM((2, 2, TILE, 256), BF16),
                pltpu.VMEM((2, 2, TILE, 256), BF16),
                pltpu.VMEM((2, 4, 16, 256), BF16),
                dma((2, 8)), dma((2, 8)), dma((2,)), dma((5,)),
            ],
            compiler_params=pltpu.CompilerParams(collective_id=0, has_side_effects=True, vmem_limit_bytes=52 * 1024 * 1024),
        )(frames, w_in, w_rec, gate_bias, h_init, c_init)
        hidden = pltpu.with_memory_space_constraint(hidden, pltpu.VMEM)
        c_last = pltpu.with_memory_space_constraint(c_last, pltpu.VMEM)
        hidden, c_last = pl.pallas_call(
            store_kernel,
            out_shape=(
                jax.ShapeDtypeStruct((STEPS, TILE, TILE, C_HID), BF16),
                jax.ShapeDtypeStruct((TILE, TILE, C_HID), F32),
            ),
            in_specs=[vmem, vmem],
            out_specs=(hbm, hbm),
            scratch_shapes=[dma((STEPS + 1,))],
            compiler_params=pltpu.CompilerParams(vmem_limit_bytes=1024 * 1024),
        )(hidden, c_last)
        return hidden.reshape(STEPS, 1, TILE, TILE, C_HID), c_last.reshape(1, TILE, TILE, C_HID)

    return jax.shard_map(local_run, mesh=mesh, in_specs=(seq_spec, P(), P(), P(), state_spec, state_spec), out_specs=(seq_spec, state_spec), check_vma=False)
```

```python
import functools

import jax
import jax.numpy as jnp
from jax import lax
from jax.experimental import pallas as pl
from jax.experimental.pallas import tpu as pltpu
from jax.sharding import PartitionSpec as P

MESH = pl.DeviceIdType.MESH
F32, BF16 = jnp.float32, jnp.bfloat16

STEPS = 16
TILE = 32
C_IN, C_HID = 64, 192
LANES = 128
PITCH = 48
ROW_SETS = (range(1, 9), range(9, 17), range(17, 25), (*range(25, 31), 0, 31))
HALVES = (1, 1, 2, 2)
SPLIT3 = 8
SPLIT4 = 8
LATE = 6

UP, DOWN, LEFT, RIGHT = (-1, 0), (1, 0), (0, -1), (0, 1)
DIRS = (UP, DOWN, LEFT, RIGHT, (-1, -1), (-1, 1), (1, -1), (1, 1))


def sigmoid(x):
    return 0.5 * jnp.tanh(0.5 * x) + 0.5


def kernel(n_rows, n_cols, frames, w_in, w_rec, bias, h_init, c_init, hidden, c_out,
         w, lhs, st0, st1, c0, c1, ge, gp, ce, cv, fb, hb, bb, ci, cs, row_in, col_in, diag_in,
         send_sem, recv_sem, frame_sem, load_sem):
    my_row, my_col = lax.axis_index("rows"), lax.axis_index("cols")

    def there(d):
        r, c = my_row + d[0], my_col + d[1]
        return (r >= 0) & (r < n_rows) & (c >= 0) & (c < n_cols)

    def device(d):
        return {"rows": my_row + d[0], "cols": my_col + d[1]}

    load_w0 = pltpu.make_async_copy(w_rec, w.at[:, 0:C_HID, :], load_sem.at[0])
    load_w1 = pltpu.make_async_copy(w_in, w.at[:, C_HID:256, :], load_sem.at[1])
    load_h = pltpu.make_async_copy(h_init, hb, load_sem.at[2])
    load_c = pltpu.make_async_copy(c_init, ci, load_sem.at[3])

    def frame_copy(t, slot):
        return pltpu.make_async_copy(frames.at[t], fb.at[slot], frame_sem.at[slot])

    load_b = pltpu.make_async_copy(bias, bb, load_sem.at[4])
    load_h.start()
    load_b.start()
    frame_copy(0, 0).start()
    load_c.start()
    load_w0.start()
    load_w1.start()
    frame_copy(1, 1).start()

    row_in[...] = jnp.zeros_like(row_in)
    col_in[...] = jnp.zeros_like(col_in)
    diag_in[...] = jnp.zeros_like(diag_in)
    gp[...] = jnp.zeros_like(gp)
    for k in range(TILE + 2):
        for st in (st0, st1):
            st[pl.ds(k * PITCH, 8), :] = jnp.zeros((8, LANES), F32)
            st[pl.ds(k * PITCH + 40, 8), :] = jnp.zeros((8, LANES), F32)

    barrier = pltpu.get_barrier_semaphore()
    for d in DIRS:
        @pl.when(there(d))
        def _():
            pl.semaphore_signal(barrier, inc=1, device_id=device(d), device_id_type=MESH)
    def near(i, n):
        return 1 + (i > 0).astype(jnp.int32) + (i < n - 1).astype(jnp.int32)

    pl.semaphore_wait(barrier, near(my_row, n_rows) * near(my_col, n_cols) - 1)

    lane = lax.broadcasted_iota(jnp.int32, (TILE, LANES), 1)
    low = lane < C_IN
    cell_at = lax.broadcasted_iota(jnp.int32, (TILE, LANES), 0)

    def frame_row(slot, r):
        x = fb[slot, r].astype(F32)
        return jnp.concatenate([x, x], axis=1)

    load_h.wait()
    frame_copy(0, 0).wait()
    for r in range(TILE):
        st0[pl.ds(r * PITCH + 8, TILE), :] = hb[r, :, 0:LANES].astype(F32)
        h1 = hb[r, :, LANES:C_HID].astype(F32)
        st1[pl.ds(r * PITCH + 8, TILE), :] = jnp.where(low, jnp.concatenate([h1, h1], axis=1), frame_row(0, r))
    load_b.wait()
    load_c.wait()
    for r in range(TILE):
        c0[pl.ds(r * TILE, TILE), :] = ci[r, :, 0:LANES]
        v = ci[r, :, LANES:C_HID]
        c1[pl.ds(r * TILE, TILE), :] = jnp.concatenate([v, v], axis=1)
    for side in range(2):
        ce[side, 0] = c0[pl.ds((TILE - 1) * side, TILE, stride=TILE), :]
        ce[side, 1] = c1[pl.ds((TILE - 1) * side, TILE, stride=TILE), :]
        at = pl.ds(8 + (TILE - 1) * side, TILE, stride=PITCH)
        cs[side, :, 0:LANES] = st0[at, :].astype(BF16)
        cs[side, :, LANES:256] = st1[at, :].astype(BF16)

    def build_row(r, out_slot):
        target = r + 1 if r < TILE else (0 if r == TILE else TILE + 1)
        for dx in range(3):
            v0 = st0[pl.ds(r * PITCH + 7 + dx, TILE), :].astype(BF16)
            v1 = st1[pl.ds(r * PITCH + 7 + dx, TILE), :].astype(BF16)
            if dx != 1 or r not in (0, TILE - 1):
                lhs[dx, target, :, 0:LANES] = v0
                lhs[dx, target, :, LANES:256] = v1
            if dx == 1 and out_slot is not None:
                hidden[out_slot, r, :, 0:LANES] = v0
                hidden[out_slot, r, :, LANES:C_HID] = v1[:, 0:C_IN]

    def cell(gates, c0_prev, c1_prev):
        s0, s1, s2, s3 = (sigmoid(gates[k]) for k in range(4))
        scale = jnp.where(low, 0.5, 1.0)
        t4 = jnp.tanh(gates[4] * scale) * scale + jnp.where(low, 0.5, 0.0)
        t5 = jnp.tanh(gates[5])
        r1, r2, r4, r5 = (pltpu.roll(v, 64, 1) for v in (s1, s2, t4, t5))
        c0_next = jnp.where(low, r1, r2) * c0_prev + s0 * jnp.where(low, r4, r5)
        c1_next = r2 * c1_prev + s1 * r5
        return s3 * jnp.tanh(c0_next), t4 * jnp.tanh(c1_next), c0_next, c1_next

    def bias_piece(k):
        return bb[k * LANES:(k + 1) * LANES].reshape(1, LANES)

    def products(rows, halves, taps):
        x = [jnp.concatenate([lhs[tap % 3, r + tap // 3] for r in rows], axis=0) for tap in taps]
        x = jnp.concatenate(x, axis=1)
        weights = w[taps[0]:taps[-1] + 1].reshape(len(taps) * 256, 4 * C_HID)
        size = x.shape[0] // halves
        rest = [jnp.dot(x[k * size:(k + 1) * size], weights[:, 512:], preferred_element_type=F32) for k in range(halves)]
        return [jnp.dot(x, weights[:, 0:512], preferred_element_type=F32)] + rest

    def whole(parts):
        return parts[0], jnp.concatenate(parts[1:], axis=0)

    def chunk_gates(rows, halves):
        return whole(products(rows, halves, range(9)))

    def gate_row(gates, j, r):
        pre = jnp.concatenate([g[j * TILE:(j + 1) * TILE] for g in gates], axis=1)
        pre = [pre[:, k * LANES:(k + 1) * LANES] + bias_piece(k) for k in range(6)]
        for k in range(6):
            ge[0, k, pl.ds(r * 8, 8), :] = pre[k][0:8]
            ge[1, k, pl.ds(r * 8, 8), :] = pre[k][24:32]
        return pre

    def cell_row(gates, j, r, x_slot):
        pre = gate_row(gates, j, r)
        at = pl.ds(r * TILE, TILE)
        h0, h1, c0_next, c1_next = cell(pre, c0[at, :], c1[at, :])
        c0[at, :] = c0_next
        c1[at, :] = c1_next
        st0[pl.ds(r * PITCH + 8, TILE), :] = h0
        st1[pl.ds(r * PITCH + 8, TILE), :] = jnp.where(low, h1, frame_row(x_slot, r))

    def cell_row_late(j, r, t):
        at = pl.ds(r * TILE, TILE)
        here = pl.ds(r * PITCH + 8, TILE)
        live = jnp.full((TILE, LANES), t, jnp.int32) > 0
        inner = live & (cell_at > 0) & (cell_at < TILE - 1)
        h0, h1, c0_next, c1_next = cell([gp[j, k] for k in range(6)], c0[at, :], c1[at, :])
        c0[at, :] = jnp.where(live, c0_next, c0[at, :])
        c1[at, :] = jnp.where(live, c1_next, c1[at, :])
        st0[here, :] = jnp.where(inner, h0, st0[here, :])
        st1[here, :] = jnp.where(inner & low, h1, st1[here, :])

    def sends(slot):
        pieces = (
            (UP, lhs.at[1, 1], row_in.at[slot, 1]),
            (DOWN, lhs.at[1, TILE], row_in.at[slot, 0]),
            (LEFT, cs.at[0], col_in.at[slot, 1]),
            (RIGHT, cs.at[1], col_in.at[slot, 0]),
            ((-1, -1), cs.at[0, 0:16], diag_in.at[slot, 3]),
            ((-1, 1), cs.at[1, 0:16], diag_in.at[slot, 2]),
            ((1, -1), cs.at[0, 16:32], diag_in.at[slot, 1]),
            ((1, 1), cs.at[1, 16:32], diag_in.at[slot, 0]),
        )
        return [(d, pltpu.make_async_remote_copy(
            src_ref=src, dst_ref=dst, send_sem=send_sem.at[slot, k], recv_sem=recv_sem.at[slot, k],
            device_id=device(d), device_id_type=MESH)) for k, (d, src, dst) in enumerate(pieces)]

    def wait_recv(copies, which):
        for k in which:
            d, copy = copies[k]
            @pl.when(there((-d[0], -d[1])))
            def _():
                copy.wait_recv()

    def step(t, _):
        slot = lax.rem(t, 2)
        x_slot = lax.rem(t + 1, 2)
        copies = sends(slot)

        done = lax.rem(t + STEPS - 1, STEPS)
        for r in (0, TILE - 1):
            here = pl.ds(r * PITCH + 8, TILE)
            lhs[1, r + 1, :, 0:LANES] = st0[here, :].astype(BF16)
            lhs[1, r + 1, :, LANES:256] = st1[here, :].astype(BF16)
        for d, copy in copies[2:] + copies[:2]:
            @pl.when(there(d))
            def _():
                copy.start()

        @pl.when(t < STEPS - 2)
        def _():
            frame_copy(t + 2, slot).start()
        @pl.when(t < STEPS - 1)
        def _():
            frame_copy(t + 1, x_slot).wait()

        @pl.when(t == 0)
        def _():
            load_w0.wait()
            load_w1.wait()

        built = 0
        before = None
        for i, rows in enumerate(ROW_SETS[:-1]):
            top = min(max(rows) + 2, TILE)
            for r in range(built, top):
                build_row(r, done)
            built = top
            if i < len(ROW_SETS) - 2:
                gates = chunk_gates(rows, HALVES[i])
            else:
                gates = products(rows, HALVES[i], range(SPLIT3))
            if i == 0:
                for j in range(LATE):
                    cell_row_late(j, ROW_SETS[-1][j], t)
            if before is not None:
                for j, r in enumerate(ROW_SETS[i - 1]):
                    cell_row(before, j, r, x_slot)
            before = gates
        for r in range(built, TILE):
            build_row(r, done)

        wait_recv(copies, (0, 1))
        rest = products(ROW_SETS[-2], HALVES[-2], range(SPLIT3, 9))
        before = whole([b + a for a, b in zip(before, rest)])
        for k in range(2):
            at = pl.ds((TILE + k) * PITCH + 8, TILE)
            st0[at, :] = row_in[slot, k, :, 0:LANES].astype(F32)
            st1[at, :] = row_in[slot, k, :, LANES:256].astype(F32)
            build_row(TILE + k, None)
        more = products(ROW_SETS[-1], HALVES[-1], range(SPLIT4))
        for j, r in enumerate(ROW_SETS[-2]):
            cell_row(before, j, r, x_slot)

        for d, copy in copies:
            @pl.when(there(d))
            def _():
                copy.wait_send()
        wait_recv(copies, range(2, 8))
        rest = products(ROW_SETS[-1], HALVES[-1], range(SPLIT4, 9))
        more = whole([b + a for a, b in zip(more, rest)])
        for side in range(2):
            for k in range(2):
                part = slice(k * LANES, (k + 1) * LANES)
                cv[side, k, 8:40, :] = col_in[slot, side, :, part].astype(F32)
                cv[side, k, 7:8, :] = diag_in[slot, side, 15:16, part].astype(F32)
                cv[side, k, 40:41, :] = diag_in[slot, 2 + side, 0:1, part].astype(F32)
        extra = []
        for side in range(2):
            halo = jnp.concatenate([cv[side, k, 7 + dy:39 + dy, :].astype(BF16) for dy in range(3) for k in range(2)], axis=1)
            taps = jnp.concatenate([w[dy * 3 + 2 * side] for dy in range(3)], axis=0)
            extra.append(jnp.dot(halo, taps, preferred_element_type=F32))
        for j, r in enumerate(ROW_SETS[-1]):
            if j < LATE:
                for k, v in enumerate(gate_row(more, j, r)):
                    gp[j, k] = v
                st1[pl.ds(r * PITCH + 8, TILE), :] = frame_row(x_slot, r)
            else:
                cell_row(more, j, r, x_slot)
        for side in range(2):
            more = [extra[side][:, k * LANES:(k + 1) * LANES] for k in range(6)]
            pre = [ge[side, k, pl.ds(7 * side, TILE, stride=8), :] + more[k] for k in range(6)]
            h0, h1, c0_next, c1_next = cell(pre, ce[side, 0], ce[side, 1])
            ce[side, 0] = c0_next
            ce[side, 1] = c1_next
            at = pl.ds(8 + (TILE - 1) * side, TILE, stride=PITCH)
            h1 = jnp.where(low, h1, st1[at, :])
            st0[at, :] = h0
            st1[at, :] = h1
            cs[side, :, 0:LANES] = h0.astype(BF16)
            cs[side, :, LANES:256] = h1.astype(BF16)
        return 0

    lax.fori_loop(0, STEPS, step, 0)

    for j in range(LATE):
        cell_row_late(j, ROW_SETS[-1][j], STEPS)
    for r in range(TILE):
        at = pl.ds(r * PITCH + 8, TILE)
        hidden[STEPS - 1, r, :, 0:LANES] = st0[at, :].astype(BF16)
        hidden[STEPS - 1, r, :, LANES:C_HID] = st1[at, :].astype(BF16)[:, 0:C_IN]
    for side in range(2):
        c0[pl.ds((TILE - 1) * side, TILE, stride=TILE), :] = ce[side, 0]
        c1[pl.ds((TILE - 1) * side, TILE, stride=TILE), :] = ce[side, 1]
    for r in range(TILE):
        at = pl.ds(r * TILE, TILE)
        c_out[r, :, 0:LANES] = c0[at, :]
        c_out[r, :, LANES:C_HID] = c1[at, :][:, 0:C_IN]


def store_kernel(hidden, c_last, hidden_out, c_out, sem):
    copies = [pltpu.make_async_copy(c_last, c_out, sem.at[STEPS])]
    copies += [pltpu.make_async_copy(hidden.at[t], hidden_out.at[t], sem.at[t]) for t in range(STEPS)]
    for copy in copies:
        copy.start()
    for copy in copies:
        copy.wait()


def solution(mesh):
    n_rows = mesh.shape["rows"]
    n_cols = mesh.shape["cols"]
    seq_spec = P(None, "dp", "rows", "cols", None)
    state_spec = P("dp", "rows", "cols", None)

    def local_run(frames, w_in, w_rec, gate_bias, h_init, c_init):
        frames = frames.reshape(STEPS, TILE, TILE, C_IN)
        w_in = w_in.reshape(9, C_IN, 4 * C_HID)
        w_rec = w_rec.reshape(9, C_HID, 4 * C_HID)
        h_init = h_init.reshape(TILE, TILE, C_HID)
        c_init = c_init.reshape(TILE, TILE, C_HID)
        hbm = pl.BlockSpec(memory_space=pltpu.HBM)
        vmem = pl.BlockSpec(memory_space=pltpu.VMEM)
        dma = pltpu.SemaphoreType.DMA
        hidden, c_last = pl.pallas_call(
            functools.partial(kernel, n_rows, n_cols),
            out_shape=(
                pltpu.VMEM((STEPS, TILE, TILE, C_HID), BF16),
                pltpu.VMEM((TILE, TILE, C_HID), F32),
            ),
            in_specs=[hbm] * 6,
            out_specs=(vmem, vmem),
            scratch_shapes=[
                pltpu.VMEM((9, 256, 4 * C_HID), BF16),
                pltpu.VMEM((3, TILE + 2, TILE, 256), BF16),
                pltpu.VMEM(((TILE + 2) * PITCH, LANES), F32),
                pltpu.VMEM(((TILE + 2) * PITCH, LANES), F32),
                pltpu.VMEM((TILE * TILE, LANES), F32),
                pltpu.VMEM((TILE * TILE, LANES), F32),
                pltpu.VMEM((2, 6, 8 * TILE, LANES), F32),
                pltpu.VMEM((LATE, 6, TILE, LANES), F32),
                pltpu.VMEM((2, 2, TILE, LANES), F32),
                pltpu.VMEM((2, 2, PITCH, LANES), F32),
                pltpu.VMEM((2, TILE, TILE, C_IN), BF16),
                pltpu.VMEM((TILE, TILE, C_HID), BF16),
                pltpu.VMEM((4 * C_HID,), F32),
                pltpu.VMEM((TILE, TILE, C_HID), F32),
                pltpu.VMEM((2, TILE, 256), BF16),
                pltpu.VMEM((2, 2, TILE, 256), BF16),
                pltpu.VMEM((2, 2, TILE, 256), BF16),
                pltpu.VMEM((2, 4, 16, 256), BF16),
                dma((2, 8)), dma((2, 8)), dma((2,)), dma((5,)),
            ],
            compiler_params=pltpu.CompilerParams(collective_id=0, has_side_effects=True, vmem_limit_bytes=52 * 1024 * 1024),
        )(frames, w_in, w_rec, gate_bias, h_init, c_init)
        hidden = pltpu.with_memory_space_constraint(hidden, pltpu.VMEM)
        c_last = pltpu.with_memory_space_constraint(c_last, pltpu.VMEM)
        hidden, c_last = pl.pallas_call(
            store_kernel,
            out_shape=(
                jax.ShapeDtypeStruct((STEPS, TILE, TILE, C_HID), BF16),
                jax.ShapeDtypeStruct((TILE, TILE, C_HID), F32),
            ),
            in_specs=[vmem, vmem],
            out_specs=(hbm, hbm),
            scratch_shapes=[dma((STEPS + 1,))],
            compiler_params=pltpu.CompilerParams(vmem_limit_bytes=1024 * 1024),
        )(hidden, c_last)
        return hidden.reshape(STEPS, 1, TILE, TILE, C_HID), c_last.reshape(1, TILE, TILE, C_HID)

    return jax.shard_map(local_run, mesh=mesh, in_specs=(seq_spec, P(), P(), P(), state_spec, state_spec), out_specs=(seq_spec, state_spec), check_vma=False)
```

```python
import functools

import jax
import jax.numpy as jnp
from jax import lax
from jax.experimental import pallas as pl
from jax.experimental.pallas import tpu as pltpu
from jax.sharding import PartitionSpec as P

MESH = pl.DeviceIdType.MESH
F32, BF16 = jnp.float32, jnp.bfloat16

STEPS = 16
TILE = 32
C_IN, C_HID = 64, 192
LANES = 128
PITCH = 48
ROW_SETS = (range(1, 9), range(9, 17), range(17, 25), (*range(25, 31), 0, 31))
HALVES = (1, 1, 2, 2)
SPLIT3 = 8
SPLIT4 = 8
LATE = 6

UP, DOWN, LEFT, RIGHT = (-1, 0), (1, 0), (0, -1), (0, 1)
DIRS = (UP, DOWN, LEFT, RIGHT, (-1, -1), (-1, 1), (1, -1), (1, 1))


def sigmoid(x):
    return 0.5 * jnp.tanh(0.5 * x) + 0.5


def kernel(n_rows, n_cols, frames, w_in, w_rec, bias, h_init, c_init, hidden, c_out,
         w, lhs, st0, st1, c0, c1, ge, gp, ce, cv, fb, hb, bb, ci, cs, row_in, col_in, diag_in,
         send_sem, recv_sem, frame_sem, load_sem):
    my_row, my_col = lax.axis_index("rows"), lax.axis_index("cols")

    def there(d):
        r, c = my_row + d[0], my_col + d[1]
        return (r >= 0) & (r < n_rows) & (c >= 0) & (c < n_cols)

    def device(d):
        return {"rows": my_row + d[0], "cols": my_col + d[1]}

    load_w0 = pltpu.make_async_copy(w_rec, w.at[:, 0:C_HID, :], load_sem.at[0])
    load_w1 = pltpu.make_async_copy(w_in, w.at[:, C_HID:256, :], load_sem.at[1])
    load_h = pltpu.make_async_copy(h_init, hb, load_sem.at[2])
    load_c = pltpu.make_async_copy(c_init, ci, load_sem.at[3])

    def frame_copy(t, slot):
        return pltpu.make_async_copy(frames.at[t], fb.at[slot], frame_sem.at[slot])

    load_b = pltpu.make_async_copy(bias, bb, load_sem.at[4])
    load_h.start()
    load_b.start()
    frame_copy(0, 0).start()
    load_c.start()
    load_w0.start()
    load_w1.start()
    frame_copy(1, 1).start()

    row_in[...] = jnp.zeros_like(row_in)
    col_in[...] = jnp.zeros_like(col_in)
    diag_in[...] = jnp.zeros_like(diag_in)
    gp[...] = jnp.zeros_like(gp)
    for k in range(TILE + 2):
        for st in (st0, st1):
            st[pl.ds(k * PITCH, 8), :] = jnp.zeros((8, LANES), F32)
            st[pl.ds(k * PITCH + 40, 8), :] = jnp.zeros((8, LANES), F32)

    barrier = pltpu.get_barrier_semaphore()
    for d in DIRS:
        @pl.when(there(d))
        def _():
            pl.semaphore_signal(barrier, inc=1, device_id=device(d), device_id_type=MESH)
    def near(i, n):
        return 1 + (i > 0).astype(jnp.int32) + (i < n - 1).astype(jnp.int32)

    pl.semaphore_wait(barrier, near(my_row, n_rows) * near(my_col, n_cols) - 1)

    lane = lax.broadcasted_iota(jnp.int32, (TILE, LANES), 1)
    low = lane < C_IN
    cell_at = lax.broadcasted_iota(jnp.int32, (TILE, LANES), 0)

    def frame_row(slot, r):
        x = fb[slot, r].astype(F32)
        return jnp.concatenate([x, x], axis=1)

    load_h.wait()
    frame_copy(0, 0).wait()
    for r in range(TILE):
        st0[pl.ds(r * PITCH + 8, TILE), :] = hb[r, :, 0:LANES].astype(F32)
        h1 = hb[r, :, LANES:C_HID].astype(F32)
        st1[pl.ds(r * PITCH + 8, TILE), :] = jnp.where(low, jnp.concatenate([h1, h1], axis=1), frame_row(0, r))
    load_b.wait()
    load_c.wait()
    for r in range(TILE):
        c0[pl.ds(r * TILE, TILE), :] = ci[r, :, 0:LANES]
        v = ci[r, :, LANES:C_HID]
        c1[pl.ds(r * TILE, TILE), :] = jnp.concatenate([v, v], axis=1)
    for side in range(2):
        ce[side, 0] = c0[pl.ds((TILE - 1) * side, TILE, stride=TILE), :]
        ce[side, 1] = c1[pl.ds((TILE - 1) * side, TILE, stride=TILE), :]
        at = pl.ds(8 + (TILE - 1) * side, TILE, stride=PITCH)
        cs[side, :, 0:LANES] = st0[at, :].astype(BF16)
        cs[side, :, LANES:256] = st1[at, :].astype(BF16)

    def build_row(r, out_slot):
        target = r + 1 if r < TILE else (0 if r == TILE else TILE + 1)
        for dx in range(3):
            v0 = st0[pl.ds(r * PITCH + 7 + dx, TILE), :].astype(BF16)
            v1 = st1[pl.ds(r * PITCH + 7 + dx, TILE), :].astype(BF16)
            if dx != 1 or r not in (0, TILE - 1):
                lhs[dx, target, :, 0:LANES] = v0
                lhs[dx, target, :, LANES:256] = v1
            if dx == 1 and out_slot is not None:
                hidden[out_slot, r, :, 0:LANES] = v0
                hidden[out_slot, r, :, LANES:C_HID] = v1[:, 0:C_IN]

    def cell(gates, c0_prev, c1_prev):
        s0, s1, s2, s3 = (sigmoid(gates[k]) for k in range(4))
        scale = jnp.where(low, 0.5, 1.0)
        t4 = jnp.tanh(gates[4] * scale) * scale + jnp.where(low, 0.5, 0.0)
        t5 = jnp.tanh(gates[5])
        r1, r2, r4, r5 = (pltpu.roll(v, 64, 1) for v in (s1, s2, t4, t5))
        c0_next = jnp.where(low, r1, r2) * c0_prev + s0 * jnp.where(low, r4, r5)
        c1_next = r2 * c1_prev + s1 * r5
        return s3 * jnp.tanh(c0_next), t4 * jnp.tanh(c1_next), c0_next, c1_next

    def bias_piece(k):
        return bb[k * LANES:(k + 1) * LANES].reshape(1, LANES)

    def products(rows, halves, taps):
        x = [jnp.concatenate([lhs[tap % 3, r + tap // 3] for r in rows], axis=0) for tap in taps]
        x = jnp.concatenate(x, axis=1)
        weights = w[taps[0]:taps[-1] + 1].reshape(len(taps) * 256, 4 * C_HID)
        size = x.shape[0] // halves
        rest = [jnp.dot(x[k * size:(k + 1) * size], weights[:, 512:], preferred_element_type=F32) for k in range(halves)]
        return [jnp.dot(x, weights[:, 0:512], preferred_element_type=F32)] + rest

    def whole(parts):
        return parts[0], jnp.concatenate(parts[1:], axis=0)

    def chunk_gates(rows, halves):
        return whole(products(rows, halves, range(9)))

    def gate_row(gates, j, r):
        pre = jnp.concatenate([g[j * TILE:(j + 1) * TILE] for g in gates], axis=1)
        pre = [pre[:, k * LANES:(k + 1) * LANES] + bias_piece(k) for k in range(6)]
        for k in range(6):
            ge[0, k, pl.ds(r * 8, 8), :] = pre[k][0:8]
            ge[1, k, pl.ds(r * 8, 8), :] = pre[k][24:32]
        return pre

    def cell_row(gates, j, r, x_slot):
        pre = gate_row(gates, j, r)
        at = pl.ds(r * TILE, TILE)
        h0, h1, c0_next, c1_next = cell(pre, c0[at, :], c1[at, :])
        c0[at, :] = c0_next
        c1[at, :] = c1_next
        st0[pl.ds(r * PITCH + 8, TILE), :] = h0
        st1[pl.ds(r * PITCH + 8, TILE), :] = jnp.where(low, h1, frame_row(x_slot, r))

    def cell_row_late(j, r, t):
        at = pl.ds(r * TILE, TILE)
        here = pl.ds(r * PITCH + 8, TILE)
        live = jnp.full((TILE, LANES), t, jnp.int32) > 0
        inner = live & (cell_at > 0) & (cell_at < TILE - 1)
        h0, h1, c0_next, c1_next = cell([gp[j, k] for k in range(6)], c0[at, :], c1[at, :])
        c0[at, :] = jnp.where(live, c0_next, c0[at, :])
        c1[at, :] = jnp.where(live, c1_next, c1[at, :])
        st0[here, :] = jnp.where(inner, h0, st0[here, :])
        st1[here, :] = jnp.where(inner & low, h1, st1[here, :])

    def sends(slot):
        pieces = (
            (UP, lhs.at[1, 1], row_in.at[slot, 1]),
            (DOWN, lhs.at[1, TILE], row_in.at[slot, 0]),
            (LEFT, cs.at[0], col_in.at[slot, 1]),
            (RIGHT, cs.at[1], col_in.at[slot, 0]),
            ((-1, -1), cs.at[0, 0:16], diag_in.at[slot, 3]),
            ((-1, 1), cs.at[1, 0:16], diag_in.at[slot, 2]),
            ((1, -1), cs.at[0, 16:32], diag_in.at[slot, 1]),
            ((1, 1), cs.at[1, 16:32], diag_in.at[slot, 0]),
        )
        return [(d, pltpu.make_async_remote_copy(
            src_ref=src, dst_ref=dst, send_sem=send_sem.at[slot, k], recv_sem=recv_sem.at[slot, k],
            device_id=device(d), device_id_type=MESH)) for k, (d, src, dst) in enumerate(pieces)]

    def wait_recv(copies, which):
        for k in which:
            d, copy = copies[k]
            @pl.when(there((-d[0], -d[1])))
            def _():
                copy.wait_recv()

    def step(t, _):
        slot = lax.rem(t, 2)
        x_slot = lax.rem(t + 1, 2)
        copies = sends(slot)

        done = lax.rem(t + STEPS - 1, STEPS)
        for d, copy in copies[2:]:
            @pl.when(there(d))
            def _():
                copy.start()
        for r in (0, TILE - 1):
            here = pl.ds(r * PITCH + 8, TILE)
            lhs[1, r + 1, :, 0:LANES] = st0[here, :].astype(BF16)
            lhs[1, r + 1, :, LANES:256] = st1[here, :].astype(BF16)
        for d, copy in copies[:2]:
            @pl.when(there(d))
            def _():
                copy.start()

        @pl.when(t < STEPS - 2)
        def _():
            frame_copy(t + 2, slot).start()
        @pl.when(t < STEPS - 1)
        def _():
            frame_copy(t + 1, x_slot).wait()

        @pl.when(t == 0)
        def _():
            load_w0.wait()
            load_w1.wait()

        built = 0
        before = None
        for i, rows in enumerate(ROW_SETS[:-1]):
            top = min(max(rows) + 2, TILE)
            for r in range(built, top):
                build_row(r, done)
            built = top
            if i < len(ROW_SETS) - 2:
                gates = chunk_gates(rows, HALVES[i])
            else:
                gates = products(rows, HALVES[i], range(SPLIT3))
            if i == 0:
                for j in range(LATE):
                    cell_row_late(j, ROW_SETS[-1][j], t)
            if before is not None:
                for j, r in enumerate(ROW_SETS[i - 1]):
                    cell_row(before, j, r, x_slot)
            before = gates
        for r in range(built, TILE):
            build_row(r, done)

        wait_recv(copies, (0, 1))
        rest = products(ROW_SETS[-2], HALVES[-2], range(SPLIT3, 9))
        before = whole([b + a for a, b in zip(before, rest)])
        for k in range(2):
            at = pl.ds((TILE + k) * PITCH + 8, TILE)
            st0[at, :] = row_in[slot, k, :, 0:LANES].astype(F32)
            st1[at, :] = row_in[slot, k, :, LANES:256].astype(F32)
            build_row(TILE + k, None)
        more = products(ROW_SETS[-1], HALVES[-1], range(SPLIT4))
        for j, r in enumerate(ROW_SETS[-2]):
            cell_row(before, j, r, x_slot)

        for d, copy in copies:
            @pl.when(there(d))
            def _():
                copy.wait_send()
        wait_recv(copies, range(2, 8))
        rest = products(ROW_SETS[-1], HALVES[-1], range(SPLIT4, 9))
        more = whole([b + a for a, b in zip(more, rest)])
        for side in range(2):
            for k in range(2):
                part = slice(k * LANES, (k + 1) * LANES)
                cv[side, k, 8:40, :] = col_in[slot, side, :, part].astype(F32)
                cv[side, k, 7:8, :] = diag_in[slot, side, 15:16, part].astype(F32)
                cv[side, k, 40:41, :] = diag_in[slot, 2 + side, 0:1, part].astype(F32)
        extra = []
        for side in range(2):
            halo = jnp.concatenate([cv[side, k, 7 + dy:39 + dy, :].astype(BF16) for dy in range(3) for k in range(2)], axis=1)
            taps = jnp.concatenate([w[dy * 3 + 2 * side] for dy in range(3)], axis=0)
            extra.append(jnp.dot(halo, taps, preferred_element_type=F32))
        for j, r in enumerate(ROW_SETS[-1]):
            if j < LATE:
                for k, v in enumerate(gate_row(more, j, r)):
                    gp[j, k] = v
                st1[pl.ds(r * PITCH + 8, TILE), :] = frame_row(x_slot, r)
            else:
                cell_row(more, j, r, x_slot)
        for side in range(2):
            more = [extra[side][:, k * LANES:(k + 1) * LANES] for k in range(6)]
            pre = [ge[side, k, pl.ds(7 * side, TILE, stride=8), :] + more[k] for k in range(6)]
            h0, h1, c0_next, c1_next = cell(pre, ce[side, 0], ce[side, 1])
            ce[side, 0] = c0_next
            ce[side, 1] = c1_next
            at = pl.ds(8 + (TILE - 1) * side, TILE, stride=PITCH)
            h1 = jnp.where(low, h1, st1[at, :])
            st0[at, :] = h0
            st1[at, :] = h1
            cs[side, :, 0:LANES] = h0.astype(BF16)
            cs[side, :, LANES:256] = h1.astype(BF16)
        return 0

    lax.fori_loop(0, STEPS, step, 0)

    for j in range(LATE):
        cell_row_late(j, ROW_SETS[-1][j], STEPS)
    for r in range(TILE):
        at = pl.ds(r * PITCH + 8, TILE)
        hidden[STEPS - 1, r, :, 0:LANES] = st0[at, :].astype(BF16)
        hidden[STEPS - 1, r, :, LANES:C_HID] = st1[at, :].astype(BF16)[:, 0:C_IN]
    for side in range(2):
        c0[pl.ds((TILE - 1) * side, TILE, stride=TILE), :] = ce[side, 0]
        c1[pl.ds((TILE - 1) * side, TILE, stride=TILE), :] = ce[side, 1]
    for r in range(TILE):
        at = pl.ds(r * TILE, TILE)
        c_out[r, :, 0:LANES] = c0[at, :]
        c_out[r, :, LANES:C_HID] = c1[at, :][:, 0:C_IN]


def store_kernel(hidden, c_last, hidden_out, c_out, sem):
    copies = [pltpu.make_async_copy(c_last, c_out, sem.at[STEPS])]
    copies += [pltpu.make_async_copy(hidden.at[t], hidden_out.at[t], sem.at[t]) for t in range(STEPS)]
    for copy in copies:
        copy.start()
    for copy in copies:
        copy.wait()


def solution(mesh):
    n_rows = mesh.shape["rows"]
    n_cols = mesh.shape["cols"]
    seq_spec = P(None, "dp", "rows", "cols", None)
    state_spec = P("dp", "rows", "cols", None)

    def local_run(frames, w_in, w_rec, gate_bias, h_init, c_init):
        frames = frames.reshape(STEPS, TILE, TILE, C_IN)
        w_in = w_in.reshape(9, C_IN, 4 * C_HID)
        w_rec = w_rec.reshape(9, C_HID, 4 * C_HID)
        h_init = h_init.reshape(TILE, TILE, C_HID)
        c_init = c_init.reshape(TILE, TILE, C_HID)
        hbm = pl.BlockSpec(memory_space=pltpu.HBM)
        vmem = pl.BlockSpec(memory_space=pltpu.VMEM)
        dma = pltpu.SemaphoreType.DMA
        hidden, c_last = pl.pallas_call(
            functools.partial(kernel, n_rows, n_cols),
            out_shape=(
                pltpu.VMEM((STEPS, TILE, TILE, C_HID), BF16),
                pltpu.VMEM((TILE, TILE, C_HID), F32),
            ),
            in_specs=[hbm] * 6,
            out_specs=(vmem, vmem),
            scratch_shapes=[
                pltpu.VMEM((9, 256, 4 * C_HID), BF16),
                pltpu.VMEM((3, TILE + 2, TILE, 256), BF16),
                pltpu.VMEM(((TILE + 2) * PITCH, LANES), F32),
                pltpu.VMEM(((TILE + 2) * PITCH, LANES), F32),
                pltpu.VMEM((TILE * TILE, LANES), F32),
                pltpu.VMEM((TILE * TILE, LANES), F32),
                pltpu.VMEM((2, 6, 8 * TILE, LANES), F32),
                pltpu.VMEM((LATE, 6, TILE, LANES), F32),
                pltpu.VMEM((2, 2, TILE, LANES), F32),
                pltpu.VMEM((2, 2, PITCH, LANES), F32),
                pltpu.VMEM((2, TILE, TILE, C_IN), BF16),
                pltpu.VMEM((TILE, TILE, C_HID), BF16),
                pltpu.VMEM((4 * C_HID,), F32),
                pltpu.VMEM((TILE, TILE, C_HID), F32),
                pltpu.VMEM((2, TILE, 256), BF16),
                pltpu.VMEM((2, 2, TILE, 256), BF16),
                pltpu.VMEM((2, 2, TILE, 256), BF16),
                pltpu.VMEM((2, 4, 16, 256), BF16),
                dma((2, 8)), dma((2, 8)), dma((2,)), dma((5,)),
            ],
            compiler_params=pltpu.CompilerParams(collective_id=0, has_side_effects=True, vmem_limit_bytes=52 * 1024 * 1024),
        )(frames, w_in, w_rec, gate_bias, h_init, c_init)
        hidden = pltpu.with_memory_space_constraint(hidden, pltpu.VMEM)
        c_last = pltpu.with_memory_space_constraint(c_last, pltpu.VMEM)
        hidden, c_last = pl.pallas_call(
            store_kernel,
            out_shape=(
                jax.ShapeDtypeStruct((STEPS, TILE, TILE, C_HID), BF16),
                jax.ShapeDtypeStruct((TILE, TILE, C_HID), F32),
            ),
            in_specs=[vmem, vmem],
            out_specs=(hbm, hbm),
            scratch_shapes=[dma((STEPS + 1,))],
            compiler_params=pltpu.CompilerParams(vmem_limit_bytes=1024 * 1024),
        )(hidden, c_last)
        return hidden.reshape(STEPS, 1, TILE, TILE, C_HID), c_last.reshape(1, TILE, TILE, C_HID)

    return jax.shard_map(local_run, mesh=mesh, in_specs=(seq_spec, P(), P(), P(), state_spec, state_spec), out_specs=(seq_spec, state_spec), check_vma=False)
```
